32 devices in a mesh: frame: 16 (over z, y, x), row: 2 (over core).
Axes of the slice: x: 2, y: 2, z: 4, core: 2. Of those that a mesh axis runs over, the one named last changes fastest.
Arguments:
- footage: float32 [64, 1024, 1024], P('frame', 'row'), may hold values from -30 to 30
Outputs:
- coefficients: float32 [64, 1024, 1024], P('frame', 'row')
- energies: float32 [4, 10], replicated
The draws below stay inside these ranges and needn't reach their ends.
All inputs are finite; a program needn't handle non-finite values.
Results may differ from the reference program's by a relative error of at most 0.00007.
Values sent between devices are 32-bit elements; how exact they have to be, the bound alone decides.
A program may use at most 128 MiB of HBM per device.

```python
import math
from functools import partial
import jax
import jax.numpy as jnp
import numpy as np
from jax import lax

H = 1024
W = 1024
SLEVELS = 3
TLEVELS = 3
FRAMES = 64


def draw_footage(key, part):
    subkeys = jax.random.split(jax.random.fold_in(key, 7), 1)
    full_shape = (FRAMES, H, W)
    frame_ramp = jnp.arange(FRAMES, dtype=jnp.float32) / (FRAMES - 1)
    values = jnp.clip(jax.random.normal(subkeys[0], full_shape, jnp.float32), -5.0, 5.0)
    values = values * jnp.exp(math.log(3.0) * frame_ramp)[:, None, None]
    return values


def setup_inputs(seed: int = 0) -> dict:
    keys = jax.random.split(jax.random.key(seed), 2)
    return {
        "footage": draw_footage(jax.random.fold_in(keys[1], 71), 0),
    }


LIFT_ALPHA = -1.586134342
LIFT_BETA = -0.05298011854
LIFT_GAMMA = 0.8829110762
LIFT_DELTA = 0.4435068522
LIFT_ZETA = 1.149604398


def mirror_after(values, along):
    length = values.shape[along]
    return jnp.concatenate([lax.slice_in_dim(values, 1, length, axis=along), lax.slice_in_dim(values, length - 1, length, axis=along)], axis=along)


def mirror_before(values, along):
    length = values.shape[along]
    return jnp.concatenate([lax.slice_in_dim(values, 0, 1, axis=along), lax.slice_in_dim(values, 0, length - 1, axis=along)], axis=along)


def weave_axis(even_part, odd_part, along):
    stacked = jnp.stack([even_part, odd_part], axis=along + 1)
    new_shape = list(even_part.shape)
    new_shape[along] = new_shape[along] * 2
    return stacked.reshape(tuple(new_shape))


def lift_pair(even_part, odd_part, take_next, take_prev):
    odd_part = odd_part + LIFT_ALPHA * (even_part + take_next(even_part))
    even_part = even_part + LIFT_BETA * (take_prev(odd_part) + odd_part)
    odd_part = odd_part + LIFT_GAMMA * (even_part + take_next(even_part))
    even_part = even_part + LIFT_DELTA * (take_prev(odd_part) + odd_part)
    return even_part * LIFT_ZETA, odd_part * (1.0 / LIFT_ZETA)


def spatial(planes_in, levels, take_next, take_prev):
    row_axis = planes_in.ndim - 2
    col_axis = planes_in.ndim - 1
    low_cols, high_cols = lift_pair(planes_in[..., 0::2], planes_in[..., 1::2], partial(mirror_after, along=col_axis), partial(mirror_before, along=col_axis))
    combined = jnp.concatenate([low_cols, high_cols], axis=col_axis)
    low_rows, high_rows = lift_pair(combined[..., 0::2, :], combined[..., 1::2, :], take_next, take_prev)
    half_width = low_cols.shape[-1]
    coarse = low_rows[..., :half_width]
    if levels > 1:
        coarse = spatial(coarse, levels - 1, take_next, take_prev)
    upper_rows = weave_axis(coarse, low_rows[..., half_width:], col_axis)
    bottom = weave_axis(high_rows[..., :half_width], high_rows[..., half_width:], col_axis)
    return weave_axis(upper_rows, bottom, row_axis)


def temporal(planes_in, levels):
    even_part = planes_in[0::2]
    odd_part = planes_in[1::2]
    odd_part = odd_part - 0.5 * (even_part + mirror_after(even_part, 0))
    even_part = even_part + 0.25 * (mirror_before(odd_part, 0) + odd_part)
    if levels > 1:
        even_part = temporal(even_part, levels - 1)
    return weave_axis(even_part, odd_part, 0)


def level_of(number, ceiling):
    depth_now = 1
    while number % 2 == 0 and depth_now <= ceiling:
        number = number // 2
        depth_now = depth_now + 1
    return depth_now


def space_table(levels):
    period = 2 ** levels
    band_table = np.zeros((period * period, 3 * levels + 1), np.float32)
    for row_pos in range(period):
        for col_pos in range(period):
            row_level = level_of(row_pos, levels)
            col_level = level_of(col_pos, levels)
            finest = min(row_level, col_level)
            if finest > levels:
                column = 3 * levels
            elif row_level == col_level:
                column = 3 * (finest - 1) + 2
            elif row_level == finest:
                column = 3 * (finest - 1)
            else:
                column = 3 * (finest - 1) + 1
            band_table[row_pos * period + col_pos, column] = 1.0
    return band_table


def time_table(levels):
    period = 2 ** levels
    band_table = np.zeros((period, levels + 1), np.float32)
    for number in range(period):
        band_table[number, level_of(number, levels) - 1] = 1.0
    return band_table


def band_sums(coeffs, first_frame, levels_s, levels_t):
    period = 2 ** levels_s
    frame_count, row_count, col_count = coeffs.shape
    square = coeffs * coeffs
    pattern = square.reshape(frame_count, row_count // period, period, col_count // period, period).sum(axis=(1, 3))
    pattern = pattern.reshape(frame_count, period * period)
    per_frame = jnp.dot(pattern, jnp.asarray(space_table(levels_s), jnp.float32), precision=lax.Precision.HIGHEST)
    time_period = 2 ** levels_t
    position = (first_frame + jnp.arange(frame_count, dtype=jnp.int32)) % time_period
    onehot = (position[:, None] == jnp.arange(time_period, dtype=jnp.int32)[None, :]).astype(jnp.float32)
    frame_band = jnp.dot(onehot, jnp.asarray(time_table(levels_t), jnp.float32), precision=lax.Precision.HIGHEST)
    return jnp.dot(frame_band.T, per_frame, precision=lax.Precision.HIGHEST)


def band_means(totals, frames_all, rows_all, cols_all, levels_s, levels_t):
    space_share = space_table(levels_s).sum(0) / float((2 ** levels_s) ** 2)
    time_share = time_table(levels_t).sum(0) / float(2 ** levels_t)
    counts = float(frames_all) * float(rows_all) * float(cols_all) * np.outer(time_share, space_share)
    return totals / jnp.asarray(counts, jnp.float32)


def reference(footage):
    frames_all, rows_all, cols_all = footage.shape

    def picture_step(picture):
        return spatial(picture[None], SLEVELS, partial(mirror_after, along=1), partial(mirror_before, along=1))[0]

    planes = lax.map(picture_step, footage)
    block_rows = 8
    grouped = jnp.moveaxis(planes.reshape(frames_all, rows_all // block_rows, block_rows, cols_all), 1, 0)

    def time_step(row_block):
        return temporal(row_block, TLEVELS)

    temporal_out = lax.map(time_step, grouped)
    coeffs = jnp.moveaxis(temporal_out, 0, 1).reshape(frames_all, rows_all, cols_all)
    totals = band_sums(coeffs, 0, SLEVELS, TLEVELS)
    return coeffs, band_means(totals, frames_all, rows_all, cols_all, SLEVELS, TLEVELS)
```

```python
import jax
import jax.numpy as jnp
import numpy as np
from jax import lax
from jax.experimental import pallas as pl
from jax.experimental.pallas import tpu as pltpu
from jax.sharding import PartitionSpec as P

SLEVELS = 3
TLEVELS = 3
PERIOD = 2**SLEVELS
MARGIN = 8
GROUP = 4
BLOCK = 256
LANES = 128

LIFT_ALPHA = -1.586134342
LIFT_BETA = -0.05298011854
LIFT_GAMMA = 0.8829110762
LIFT_DELTA = 0.4435068522
LIFT_ZETA = 1.149604398
STEPS = (LIFT_ALPHA, LIFT_BETA, LIFT_GAMMA, LIFT_DELTA)
MESH = pl.DeviceIdType.MESH


def level_of(number, ceiling):
    depth_now = 1
    while number % 2 == 0 and depth_now <= ceiling:
        number = number // 2
        depth_now = depth_now + 1
    return depth_now


def space_band(row_level, col_level, levels):
    finest = min(row_level, col_level)
    if finest > levels:
        return 3 * levels
    if row_level == col_level:
        return 3 * (finest - 1) + 2
    if row_level == finest:
        return 3 * (finest - 1)
    return 3 * (finest - 1) + 1


def lifted_identity(size):
    x = np.eye(size)
    after = np.concatenate([np.arange(2, size, 2), [size - 2]])
    before = np.concatenate([[1], np.arange(1, size - 1, 2)])
    even, odd = np.arange(0, size, 2), np.arange(1, size, 2)
    x[:, odd] += LIFT_ALPHA * (x[:, even] + x[:, after])
    x[:, even] += LIFT_BETA * (x[:, before] + x[:, odd])
    x[:, odd] += LIFT_GAMMA * (x[:, even] + x[:, after])
    x[:, even] += LIFT_DELTA * (x[:, before] + x[:, odd])
    x[:, even] *= LIFT_ZETA
    x[:, odd] *= 1.0 / LIFT_ZETA
    return x


def high_and_low(x):
    x = np.asarray(x, np.float32)
    high = x.astype(jnp.bfloat16)
    return np.stack([high, (x - high.astype(np.float32)).astype(jnp.bfloat16)])


def column_weights(width):
    tables = []
    for level in range(SLEVELS):
        s = 2**level
        matrix = np.eye(width)
        matrix[::s, ::s] = lifted_identity(width // s)
        middle = matrix[LANES : LANES + 2 * BLOCK, BLOCK : 2 * BLOCK]
        first = matrix[:LANES, :LANES]
        last = matrix[width - LANES :, width - LANES :]
        tables.append(high_and_low(np.concatenate([middle, np.hstack([first, last])])))
    return np.stack(tables)


def energy_tables(counted):
    lane = lax.broadcasted_iota(jnp.int32, (LANES, LANES), 0)
    column = lax.broadcasted_iota(jnp.int32, (LANES, LANES), 1)
    u = lane // (LANES // (SLEVELS + 1)) + 1
    v = jnp.full_like(lane, 1)
    for level in range(1, SLEVELS + 1):
        v = v + jnp.where(lane % 2**level == 0, 1, 0)
    finest = jnp.minimum(u, v)
    kind = jnp.where(u == v, 2, jnp.where(u == finest, 0, 1))
    band = jnp.where(finest > SLEVELS, 3 * SLEVELS, 3 * (finest - 1) + kind)
    member = jnp.where(band == column, (SLEVELS + 1) * PERIOD / LANES, 0.0)
    t = lax.broadcasted_iota(jnp.int32, (8, LANES), 0)
    s = lax.broadcasted_iota(jnp.int32, (8, LANES), 1)
    share = jnp.full((8, LANES), 1.0 / counted, jnp.float32)
    for i in range(TLEVELS + 1):
        share = jnp.where(t == i, share * float(2 ** min(i + 1, TLEVELS)), share)
    for i in range(3 * SLEVELS + 1):
        share = jnp.where(s == i, share * float(4 ** min(i // 3 + 1, SLEVELS)), share)
    return member, share


def outgoing(f):
    o = {i: f[i] if i % 4 == 1 else f[i] - 0.5 * (f[i - 1] + f[i + 1]) for i in range(1, 14, 2)}
    a = {i: f[i] + 0.25 * (o[i - 1] + o[i + 1]) for i in range(2, 13, 2)}
    p6 = a[6] - 0.5 * (a[4] + a[8])
    p10 = a[10] - 0.5 * (a[8] + a[12])
    b8 = a[8] + 0.25 * (p6 + p10)
    to_before = (f[0], o[1], a[2] - 0.5 * a[4])
    to_after = (
        f[15] - 0.5 * f[14],
        f[14] + 0.25 * o[13] - 0.5 * a[12],
        a[12] + 0.25 * p10 - 0.5 * b8,
    )
    return to_before, to_after


def temporal(f, before, after, is_first, is_last):
    o = {i: f[i] if i % 4 == 1 else f[i] - 0.5 * (f[i - 1] + f[i + 1]) for i in range(1, 14, 2)}
    f16 = jnp.where(is_last, f[14], after[0])
    o[15] = f[15] - 0.5 * (f[14] + f16)
    o[-1] = jnp.where(is_first, o[1], before[0] - 0.5 * f[0])
    a = {i: f[i] + 0.25 * (o[i - 1] + o[i + 1]) for i in range(0, 16, 2)}
    a16 = jnp.where(is_last, a[12], after[0] + 0.25 * (o[15] + after[1]))
    a[16] = a16
    p = {i: a[i] - 0.5 * (a[i - 2] + a[i + 2]) for i in range(2, 16, 4)}
    p[-2] = jnp.where(is_first, p[2], before[1] + 0.25 * o[-1] - 0.5 * a[0])
    b = {i: a[i] + 0.25 * (p[i - 2] + p[i + 2]) for i in range(0, 16, 4)}
    b[16] = jnp.where(is_last, b[8], a16 + 0.25 * (p[14] + after[2] - 0.5 * a16))
    d4 = b[4] - 0.5 * (b[0] + b[8])
    d12 = b[12] - 0.5 * (b[8] + b[16])
    dm4 = jnp.where(is_first, d4, before[2] + 0.25 * p[-2] - 0.5 * b[0])
    out = {i: o[i] for i in range(1, 16, 2)}
    out.update({i: p[i] for i in range(2, 16, 4)})
    out[4], out[12] = d4, d12
    out[0] = b[0] + 0.25 * (dm4 + d4)
    out[8] = b[8] + 0.25 * (d4 + d12)
    return out


def phase_at(q):
    half, quarter = q // 4, (q // 2) % 2
    return (
        (1 - half) * (2 * q + 1)
        + half * (1 - quarter) * (4 * (q % 2) + 2)
        + half * quarter * 4 * (q % 2)
    )


def video_kernel(x_ref, w_ref, result, energy,
                 planes, edges, high, low, buf, w_mid, w_first, w_last, held,
                 from_before, from_after, to_before, to_after, acc, packed, inbox,
                 x_sem, w_sem, e_send, e_recv, f_send, f_recv, f_own, h_send, h_recv,
                 r_send, r_recv, r_own, s_send, s_recv):
    frames, phases, inner, width = planes.shape
    groups = inner + 2 * MARGIN
    part = inner // GROUP
    kept = 1
    moved = [n for n in range(frames) if n != kept]
    me = lax.axis_index("frame")
    row = lax.axis_index("row")
    strips = lax.axis_size("row")
    count = lax.axis_size("frame")
    at_top = row == 0
    at_bottom = row == strips - 1
    member = me % GROUP
    base = me - member
    is_first = base == 0
    is_last = base == count - GROUP
    peers = [base + (member + k) % GROUP for k in range(1, GROUP)]

    all_devices = count * strips
    flat = me * strips + row

    def place(device):
        return {"frame": device // strips, "row": device % strips}

    barrier = pltpu.get_barrier_semaphore()

    def greet(j, carry):
        pl.semaphore_signal(
            barrier, inc=1, device_id=place((flat + j) % all_devices), device_id_type=MESH
        )
        return carry

    lax.fori_loop(1, all_devices, greet, 0)

    def weight_copies(level):
        sources = (
            (w_ref.at[level, :, 0 : 2 * BLOCK, :], w_mid.at[level]),
            (w_ref.at[level, :, 2 * BLOCK : 2 * BLOCK + LANES, 0:LANES],
             w_first.at[level, :, 0:LANES, 0:LANES]),
            (w_ref.at[level, :, LANES : 2 * LANES, LANES:BLOCK],
             w_first.at[level, :, 0:LANES, LANES:BLOCK]),
            (w_ref.at[level, :, 2 * LANES : 2 * BLOCK, :],
             w_first.at[level, :, LANES : LANES + BLOCK, :]),
            (w_ref.at[level, :, 2 * BLOCK : 2 * BLOCK + LANES, LANES:BLOCK],
             w_last.at[level, :, BLOCK : BLOCK + LANES, LANES:BLOCK]),
            (w_ref.at[level, :, BLOCK : BLOCK + LANES, 0:LANES],
             w_last.at[level, :, BLOCK : BLOCK + LANES, 0:LANES]),
            (w_ref.at[level, :, 0:BLOCK, :], w_last.at[level, :, 0:BLOCK, :]),
        )
        return [
            pltpu.make_async_copy(source, target, w_sem.at[level, i])
            for i, (source, target) in enumerate(sources)
        ]

    def fetch(n, p):
        return pltpu.make_async_copy(x_ref.at[n, :, p, :], planes.at[n, p], x_sem.at[n, p])

    def start_fetch(n):
        for p in range(phases):
            fetch(n, p).start()

    def edge(n, p, side):
        source = pl.ds(inner - MARGIN, MARGIN) if side == 0 else pl.ds(0, MARGIN)
        target = pl.ds(MARGIN, MARGIN) if side == 0 else pl.ds(0, MARGIN)
        return pltpu.make_async_remote_copy(
            src_ref=x_ref.at[n, source, p, :],
            dst_ref=edges.at[n, p, target, :],
            send_sem=e_send.at[side, n, p],
            recv_sem=e_recv.at[side, n, p],
            device_id={"row": row + 1 if side == 0 else row - 1},
            device_id_type=MESH,
        )

    for copy in weight_copies(0):
        copy.start()
    start_fetch(0)
    for level in range(1, SLEVELS):
        for copy in weight_copies(level):
            copy.start()
    for n in (2, 1, 3):
        start_fetch(n)

    pl.semaphore_wait(barrier, all_devices - 1)

    def every_edge(side, action):
        def one(n, carry):
            for p in range(phases):
                action(edge(n, p, side))
            return carry
        lax.fori_loop(0, frames, one, 0)

    @pl.when(jnp.logical_not(at_bottom))
    def _():
        every_edge(0, lambda copy: copy.start())

    @pl.when(jnp.logical_not(at_top))
    def _():
        every_edge(1, lambda copy: copy.start())

    def part_of(device):
        return pl.ds(pl.multiple_of((device % GROUP) * part, 8), part)

    def spot(device, n):
        return (device % GROUP) * frames + n

    def forward(n, c, k):
        peer = peers[k]
        return pltpu.make_async_remote_copy(
            src_ref=planes.at[n, c, part_of(peer), :],
            dst_ref=held.at[spot(me, n), c],
            send_sem=f_send.at[n, k, c],
            recv_sem=f_recv.at[n, k, c],
            device_id={"frame": peer},
            device_id_type=MESH,
        )

    def forward_own(n, c):
        return pltpu.make_async_copy(
            planes.at[n, c, part_of(me), :], held.at[spot(me, n), c], f_own.at[n, c]
        )

    def halo(c, side):
        return pltpu.make_async_remote_copy(
            src_ref=(to_before if side == 0 else to_after).at[c],
            dst_ref=(from_after if side == 0 else from_before).at[c],
            send_sem=h_send.at[side, c],
            recv_sem=h_recv.at[side, c],
            device_id={"frame": me - GROUP if side == 0 else me + GROUP},
            device_id_type=MESH,
        )

    def halo_sends(c, action):
        @pl.when(jnp.logical_not(is_first))
        def _():
            action(halo(c, 0))

        @pl.when(jnp.logical_not(is_last))
        def _():
            action(halo(c, 1))

    def halo_arrivals(c):
        @pl.when(jnp.logical_not(is_last))
        def _():
            halo(c, 0).wait_recv()

        @pl.when(jnp.logical_not(is_first))
        def _():
            halo(c, 1).wait_recv()

    def back(i, c, k):
        peer = peers[k]
        return pltpu.make_async_remote_copy(
            src_ref=held.at[spot(peer, moved[i]), c],
            dst_ref=result.at[moved[i], c, part_of(me), :],
            send_sem=r_send.at[i, k, c],
            recv_sem=r_recv.at[i, k, c],
            device_id={"frame": peer},
            device_id_type=MESH,
        )

    def back_own(i, c):
        return pltpu.make_async_copy(
            held.at[spot(me, moved[i]), c], result.at[moved[i], c, part_of(me), :], r_own.at[i, c]
        )

    def start_forward(n, c):
        for k in range(GROUP - 1):
            forward(n, c, k).start()
        forward_own(n, c).start()

    def split(rows, lanes, value):
        rounded = value.astype(jnp.bfloat16)
        high[rows, lanes] = rounded
        low[rows, lanes] = (value - rounded.astype(jnp.float32)).astype(jnp.bfloat16)

    everything = pl.ds(0, width)
    tile = 16

    def one_frame(step, carry):
        n = (2 * step) % 3 + 3 * (step // 3)
        for p in range(phases):
            fetch(n, p).wait()

        def take(p, carry):
            for r in range(0, inner, tile):
                rows = pl.ds(pl.multiple_of(p * groups + r, tile), tile)
                split(rows, everything, planes[n, p, pl.ds(r, tile), :])
            return carry

        lax.fori_loop(0, phases, take, 0)

        @pl.when(jnp.logical_not(at_top))
        def _():
            for p in range(phases):
                edge(n, p, 0).wait_recv()

        @pl.when(jnp.logical_not(at_bottom))
        def _():
            for p in range(phases):
                edge(n, p, 1).wait_recv()

        def take_edges(p, carry):
            rows = pl.ds(pl.multiple_of(p * groups + inner, tile), tile)
            split(rows, everything, edges[n, p])
            return carry

        lax.fori_loop(0, phases, take_edges, 0)

        for level in range(SLEVELS):
            s = 2**level
            height = groups * (phases // s)

            @pl.when(step == 0)
            def _(level=level):
                for copy in weight_copies(level):
                    copy.wait()

            for b in range(width // BLOCK):
                if b == 0:
                    w, start, depth = w_first, 0, BLOCK + LANES
                elif b == width // BLOCK - 1:
                    w, start, depth = w_last, width - BLOCK - LANES, BLOCK + LANES
                else:
                    w, start, depth = w_mid, b * BLOCK - LANES, 2 * BLOCK
                xh = high[0:height, start : start + depth]
                xl = low[0:height, start : start + depth]
                wh, wl = w[level, 0], w[level, 1]
                buf[0:height, b * BLOCK : (b + 1) * BLOCK] = jnp.dot(
                    jnp.concatenate([xh, xl, xh], axis=1),
                    jnp.concatenate([wh, wh, wl], axis=0),
                    preferred_element_type=jnp.float32,
                )

            def rows(i, carry, level=level, s=s):
                lanes = pl.ds(pl.multiple_of(i * LANES, LANES), LANES)
                lane = lax.broadcasted_iota(jnp.int32, (1, LANES), 1)
                on = lane % s == 0
                x = {
                    p: buf[pl.ds(groups * (p // s), groups), lanes] for p in range(0, phases, s)
                }
                index = lax.broadcasted_iota(jnp.int32, (groups, LANES), 0)
                first = jnp.logical_and(index == 0, at_top)
                last = jnp.logical_and(index == inner - 1, at_bottom)
                for number, factor in enumerate(STEPS):
                    c = jnp.where(on, factor, 0.0)
                    if number % 2 == 0:
                        for p in range(s, phases, 2 * s):
                            if p + s < phases:
                                after = x[p + s]
                            else:
                                after = jnp.where(last, x[p - s], pltpu.roll(x[0], groups - 1, 0))
                            x[p] = x[p] + c * (x[p - s] + after)
                    else:
                        for p in range(0, phases, 2 * s):
                            if p > 0:
                                before = x[p - s]
                            else:
                                before = jnp.where(first, x[s], pltpu.roll(x[phases - s], 1, 0))
                            x[p] = x[p] + c * (before + x[p + s])
                up = jnp.where(on, LIFT_ZETA, 1.0)
                down = jnp.where(on, 1.0 / LIFT_ZETA, 1.0)
                for p in x:
                    is_low = p % (2 * s) == 0
                    value = x[p] * (up if is_low else down)
                    if is_low and level < SLEVELS - 1:
                        split(pl.ds(groups * (p // (2 * s)), groups), lanes, value)
                    else:
                        planes[n, p, :, lanes] = value[:inner]
                return carry

            lax.fori_loop(0, width // LANES, rows, 0)

            done = [
                p for p in range(0, phases, s) if p % (2 * s) != 0 or level == SLEVELS - 1
            ]

            @pl.when(step != 2)
            def _(done=done):
                for c in done:
                    start_forward(n, c)

        @pl.when(step == 2)
        def _():
            def high_frame(q, carry):
                c = phase_at(q)
                high_part = planes[kept, c] - 0.5 * (planes[kept - 1, c] + planes[kept + 1, c])
                planes[kept, c] = high_part
                result[kept, c] = high_part
                start_forward(kept, c)
                return carry

            lax.fori_loop(0, phases, high_frame, 0)

        return carry

    lax.fori_loop(0, frames, one_frame, 0)
    total = GROUP * frames

    def send_halo(q):
        c = phase_at(q)
        for n in range(frames):
            for k in range(GROUP - 1):
                forward(n, c, k).wait_recv()
            forward_own(n, c).wait()

        def strip(i, carry):
            lanes = pl.ds(pl.multiple_of(i * LANES, LANES), LANES)
            left, right = outgoing([held[n, c, :, lanes] for n in range(total)])
            for j in range(TLEVELS):
                to_before[c, j, :, lanes] = left[j]
                to_after[c, j, :, lanes] = right[j]
            return carry

        lax.fori_loop(0, width // LANES, strip, 0)
        halo_sends(c, lambda copy: copy.start())

    def finish(q):
        c = phase_at(q)
        halo_arrivals(c)

        def strip(i, carry):
            lanes = pl.ds(pl.multiple_of(i * LANES, LANES), LANES)
            f = [held[n, c, :, lanes] for n in range(total)]
            before = [from_before[c, j, :, lanes] for j in range(TLEVELS)]
            after = [from_after[c, j, :, lanes] for j in range(TLEVELS)]
            out = temporal(f, before, after, is_first, is_last)
            sums = [None] * (TLEVELS + 1)
            for n in range(total):
                if n % frames in moved:
                    held[n, c, :, lanes] = out[n]
                t = level_of(n % 2**TLEVELS, TLEVELS) - 1
                square = out[n] * out[n]
                sums[t] = square if sums[t] is None else sums[t] + square
            return tuple(
                carry[t] + jnp.sum(sums[t].reshape(part // 8, 8, LANES), axis=0)
                for t in range(TLEVELS + 1)
            )

        zero = jnp.zeros((8, LANES), jnp.float32)
        sums = lax.fori_loop(0, width // LANES, strip, (zero,) * (TLEVELS + 1))
        for t in range(TLEVELS + 1):
            acc[c, t] = sums[t]
        for i in range(len(moved)):
            for k in range(GROUP - 1):
                back(i, c, k).start()
            back_own(i, c).start()

    send_halo(0)

    def middle(q, carry):
        send_halo(q)
        finish(q - 1)
        return carry

    lax.fori_loop(1, phases, middle, 0)
    finish(phases - 1)

    lane = lax.broadcasted_iota(jnp.int32, (1, LANES), 1)
    packed[...] = jnp.zeros_like(packed)
    for t in range(TLEVELS + 1):
        line = jnp.zeros((1, LANES), jnp.float32)
        for u in range(1, SLEVELS + 2):
            mine = sum(acc[c, t] for c in range(phases) if level_of(c, SLEVELS) == u)
            mine = jnp.sum(mine, axis=0, keepdims=True)
            distance = PERIOD
            while distance < LANES:
                mine = mine + pltpu.roll(mine, distance, 1)
                distance = 2 * distance
            line = jnp.where(lane // (LANES // (SLEVELS + 1)) == u - 1, mine, line)
        packed[pl.ds(t, 1), :] = line

    def to_other(j):
        return pltpu.make_async_remote_copy(
            src_ref=packed,
            dst_ref=inbox.at[flat],
            send_sem=s_send.at[j],
            recv_sem=s_recv.at[flat],
            device_id=place((flat + j) % all_devices),
            device_id_type=MESH,
        )

    def start_sums(j, carry):
        to_other(j).start()
        return carry

    lax.fori_loop(1, all_devices, start_sums, 0)
    inbox[flat] = packed[...]

    def arrive(j, carry):
        source = (flat + j) % all_devices
        pltpu.make_async_remote_copy(
            src_ref=packed,
            dst_ref=inbox.at[source],
            send_sem=s_send.at[j],
            recv_sem=s_recv.at[source],
            device_id=place(source),
            device_id_type=MESH,
        ).wait_recv()
        return carry

    lax.fori_loop(1, all_devices, arrive, 0)
    sums = lax.fori_loop(1, all_devices, lambda j, s: s + inbox[j], inbox[0])
    counted = float(count * frames * strips * inner * phases * width)
    band, share = energy_tables(counted)
    energy[...] = share * jnp.dot(
        sums, band, precision=lax.Precision.HIGHEST, preferred_element_type=jnp.float32
    )

    def drain(c, carry):
        for k in range(GROUP - 1):
            for n in range(frames):
                forward(n, c, k).wait_send()
            for i in range(len(moved)):
                back(i, c, k).wait()
        halo_sends(c, lambda copy: copy.wait_send())
        for i in range(len(moved)):
            back_own(i, c).wait()
        return carry

    lax.fori_loop(0, phases, drain, 0)

    @pl.when(jnp.logical_not(at_bottom))
    def _():
        every_edge(0, lambda copy: copy.wait_send())

    @pl.when(jnp.logical_not(at_top))
    def _():
        every_edge(1, lambda copy: copy.wait_send())

    def drain_sums(j, carry):
        to_other(j).wait_send()
        return carry

    lax.fori_loop(1, all_devices, drain_sums, 0)


def weave_kernel(planes, energy, o_ref, e_ref, sem):
    frames, phases = planes.shape[:2]
    copies = [
        pltpu.make_async_copy(planes.at[n, p], o_ref.at[n, :, p, :], sem.at[n, p])
        for n in range(frames)
        for p in range(phases)
    ]
    for copy in copies:
        copy.start()
    e_ref[...] = energy[: TLEVELS + 1, : 3 * SLEVELS + 1]
    for copy in copies:
        copy.wait()


def shards(footage):
    frames, rows, width = footage.shape
    inner = rows // PERIOD
    groups = inner + 2 * MARGIN
    part = inner // GROUP
    strips = lax.axis_size("row")
    devices = lax.axis_size("frame") * strips
    any_space = pl.BlockSpec(memory_space=pl.ANY)
    vmem = pl.BlockSpec(memory_space=pltpu.VMEM)
    f32, bf16 = jnp.float32, jnp.bfloat16
    halo_buffer = pltpu.VMEM((PERIOD, TLEVELS, part, width), f32)
    dma = pltpu.SemaphoreType.DMA
    sent = frames - 1
    planes, energy = pl.pallas_call(
        video_kernel,
        out_shape=(
            jax.ShapeDtypeStruct((frames, PERIOD, inner, width), f32),
            jax.ShapeDtypeStruct((8, LANES), f32),
        ),
        in_specs=[any_space, pl.BlockSpec(memory_space=pltpu.HBM)],
        out_specs=(vmem, vmem),
        scratch_shapes=[
            pltpu.VMEM((frames, PERIOD, inner, width), f32),
            pltpu.VMEM((frames, PERIOD, 2 * MARGIN, width), f32),
            pltpu.VMEM((PERIOD * groups, width), bf16),
            pltpu.VMEM((PERIOD * groups, width), bf16),
            pltpu.VMEM((PERIOD * groups, width), f32),
            pltpu.VMEM((SLEVELS, 2, 2 * BLOCK, BLOCK), bf16),
            pltpu.VMEM((SLEVELS, 2, BLOCK + LANES, BLOCK), bf16),
            pltpu.VMEM((SLEVELS, 2, BLOCK + LANES, BLOCK), bf16),
            pltpu.VMEM((GROUP * frames, PERIOD, part, width), f32),
            halo_buffer, halo_buffer, halo_buffer, halo_buffer,
            pltpu.VMEM((PERIOD, TLEVELS + 1, 8, LANES), f32),
            pltpu.VMEM((8, LANES), f32),
            pltpu.VMEM((devices, 8, LANES), f32),
            dma((frames, PERIOD)), dma((SLEVELS, 7)),
            dma((2, frames, PERIOD)), dma((2, frames, PERIOD)),
            dma((frames, GROUP - 1, PERIOD)), dma((frames, GROUP - 1, PERIOD)),
            dma((frames, PERIOD)),
            dma((2, PERIOD)), dma((2, PERIOD)),
            dma((sent, GROUP - 1, PERIOD)), dma((sent, GROUP - 1, PERIOD)),
            dma((sent, PERIOD)),
            dma((devices,)), dma((devices,)),
        ],
        compiler_params=pltpu.CompilerParams(
            collective_id=0, has_side_effects=True, vmem_limit_bytes=40 * 2**20
        ),
    )(
        footage.reshape(frames, inner, PERIOD, width),
        jnp.asarray(column_weights(width)),
    )
    coeffs, means = pl.pallas_call(
        weave_kernel,
        out_shape=(
            jax.ShapeDtypeStruct((frames, inner, PERIOD, width), f32),
            jax.ShapeDtypeStruct((TLEVELS + 1, 3 * SLEVELS + 1), f32),
        ),
        in_specs=[vmem, vmem],
        out_specs=(any_space, vmem),
        scratch_shapes=[dma((frames, PERIOD))],
        compiler_params=pltpu.CompilerParams(vmem_limit_bytes=20 * 2**20),
    )(planes, energy)
    return coeffs.reshape(frames, rows, width), means


def solution(mesh):
    return jax.shard_map(
        shards,
        mesh=mesh,
        in_specs=(P("frame", "row", None),),
        out_specs=(P("frame", "row", None), P()),
        check_vma=False,
    )
```

```python
import jax
import jax.numpy as jnp
import numpy as np
from jax import lax
from jax.experimental import pallas as pl
from jax.experimental.pallas import tpu as pltpu
from jax.sharding import PartitionSpec as P

SLEVELS = 3
TLEVELS = 3
PERIOD = 2**SLEVELS
MARGIN = 8
GROUP = 4
BLOCK = 256
LANES = 128

LIFT_ALPHA = -1.586134342
LIFT_BETA = -0.05298011854
LIFT_GAMMA = 0.8829110762
LIFT_DELTA = 0.4435068522
LIFT_ZETA = 1.149604398
STEPS = (LIFT_ALPHA, LIFT_BETA, LIFT_GAMMA, LIFT_DELTA)
MESH = pl.DeviceIdType.MESH


def level_of(number, ceiling):
    depth_now = 1
    while number % 2 == 0 and depth_now <= ceiling:
        number = number // 2
        depth_now = depth_now + 1
    return depth_now


def space_band(row_level, col_level, levels):
    finest = min(row_level, col_level)
    if finest > levels:
        return 3 * levels
    if row_level == col_level:
        return 3 * (finest - 1) + 2
    if row_level == finest:
        return 3 * (finest - 1)
    return 3 * (finest - 1) + 1


def lifted_identity(size):
    x = np.eye(size)
    after = np.concatenate([np.arange(2, size, 2), [size - 2]])
    before = np.concatenate([[1], np.arange(1, size - 1, 2)])
    even, odd = np.arange(0, size, 2), np.arange(1, size, 2)
    x[:, odd] += LIFT_ALPHA * (x[:, even] + x[:, after])
    x[:, even] += LIFT_BETA * (x[:, before] + x[:, odd])
    x[:, odd] += LIFT_GAMMA * (x[:, even] + x[:, after])
    x[:, even] += LIFT_DELTA * (x[:, before] + x[:, odd])
    x[:, even] *= LIFT_ZETA
    x[:, odd] *= 1.0 / LIFT_ZETA
    return x


def high_and_low(x):
    x = np.asarray(x, np.float32)
    high = x.astype(jnp.bfloat16)
    return np.stack([high, (x - high.astype(np.float32)).astype(jnp.bfloat16)])


def column_weights(width):
    tables = []
    for level in range(SLEVELS):
        s = 2**level
        matrix = np.eye(width)
        matrix[::s, ::s] = lifted_identity(width // s)
        middle = matrix[LANES : LANES + 2 * BLOCK, BLOCK : 2 * BLOCK]
        first = matrix[:LANES, :LANES]
        last = matrix[width - LANES :, width - LANES :]
        tables.append(high_and_low(np.concatenate([middle, np.hstack([first, last])])))
    return np.stack(tables)


def energy_tables(counted):
    lane = lax.broadcasted_iota(jnp.int32, (LANES, LANES), 0)
    column = lax.broadcasted_iota(jnp.int32, (LANES, LANES), 1)
    u = lane // (LANES // (SLEVELS + 1)) + 1
    v = jnp.full_like(lane, 1)
    for level in range(1, SLEVELS + 1):
        v = v + jnp.where(lane % 2**level == 0, 1, 0)
    finest = jnp.minimum(u, v)
    kind = jnp.where(u == v, 2, jnp.where(u == finest, 0, 1))
    band = jnp.where(finest > SLEVELS, 3 * SLEVELS, 3 * (finest - 1) + kind)
    member = jnp.where(band == column, (SLEVELS + 1) * PERIOD / LANES, 0.0)
    t = lax.broadcasted_iota(jnp.int32, (8, LANES), 0)
    s = lax.broadcasted_iota(jnp.int32, (8, LANES), 1)
    share = jnp.full((8, LANES), 1.0 / counted, jnp.float32)
    for i in range(TLEVELS + 1):
        share = jnp.where(t == i, share * float(2 ** min(i + 1, TLEVELS)), share)
    for i in range(3 * SLEVELS + 1):
        share = jnp.where(s == i, share * float(4 ** min(i // 3 + 1, SLEVELS)), share)
    return member, share


def outgoing(f):
    o = {i: f[i] if i % 4 == 1 else f[i] - 0.5 * (f[i - 1] + f[i + 1]) for i in range(1, 14, 2)}
    a = {i: f[i] + 0.25 * (o[i - 1] + o[i + 1]) for i in range(2, 13, 2)}
    p6 = a[6] - 0.5 * (a[4] + a[8])
    p10 = a[10] - 0.5 * (a[8] + a[12])
    b8 = a[8] + 0.25 * (p6 + p10)
    to_before = (f[0], o[1], a[2] - 0.5 * a[4])
    to_after = (
        f[15] - 0.5 * f[14],
        f[14] + 0.25 * o[13] - 0.5 * a[12],
        a[12] + 0.25 * p10 - 0.5 * b8,
    )
    return to_before, to_after


def temporal(f, before, after, is_first, is_last):
    o = {i: f[i] if i % 4 == 1 else f[i] - 0.5 * (f[i - 1] + f[i + 1]) for i in range(1, 14, 2)}
    f16 = jnp.where(is_last, f[14], after[0])
    o[15] = f[15] - 0.5 * (f[14] + f16)
    o[-1] = jnp.where(is_first, o[1], before[0] - 0.5 * f[0])
    a = {i: f[i] + 0.25 * (o[i - 1] + o[i + 1]) for i in range(0, 16, 2)}
    a16 = jnp.where(is_last, a[12], after[0] + 0.25 * (o[15] + after[1]))
    a[16] = a16
    p = {i: a[i] - 0.5 * (a[i - 2] + a[i + 2]) for i in range(2, 16, 4)}
    p[-2] = jnp.where(is_first, p[2], before[1] + 0.25 * o[-1] - 0.5 * a[0])
    b = {i: a[i] + 0.25 * (p[i - 2] + p[i + 2]) for i in range(0, 16, 4)}
    b[16] = jnp.where(is_last, b[8], a16 + 0.25 * (p[14] + after[2] - 0.5 * a16))
    d4 = b[4] - 0.5 * (b[0] + b[8])
    d12 = b[12] - 0.5 * (b[8] + b[16])
    dm4 = jnp.where(is_first, d4, before[2] + 0.25 * p[-2] - 0.5 * b[0])
    out = {i: o[i] for i in range(1, 16, 2)}
    out.update({i: p[i] for i in range(2, 16, 4)})
    out[4], out[12] = d4, d12
    out[0] = b[0] + 0.25 * (dm4 + d4)
    out[8] = b[8] + 0.25 * (d4 + d12)
    return out


def phase_at(q):
    half, quarter = q // 4, (q // 2) % 2
    return (
        (1 - half) * (2 * q + 1)
        + half * (1 - quarter) * (4 * (q % 2) + 2)
        + half * quarter * 4 * (q % 2)
    )


def video_kernel(x_ref, w_ref, result, energy,
                 planes, edges, high, low, buf, w_mid, w_first, w_last, held,
                 from_before, from_after, to_before, to_after, acc, packed, inbox,
                 x_sem, w_sem, e_send, e_recv, f_send, f_recv, f_own, h_send, h_recv,
                 r_send, r_recv, r_own, s_send, s_recv):
    frames, phases, inner, width = planes.shape
    groups = inner + 2 * MARGIN
    part = inner // GROUP
    kept = 1
    moved = [n for n in range(frames) if n != kept]
    me = lax.axis_index("frame")
    row = lax.axis_index("row")
    strips = lax.axis_size("row")
    count = lax.axis_size("frame")
    at_top = row == 0
    at_bottom = row == strips - 1
    member = me % GROUP
    base = me - member
    is_first = base == 0
    is_last = base == count - GROUP
    peers = [base + (member + k) % GROUP for k in range(1, GROUP)]

    all_devices = count * strips
    flat = me * strips + row

    def place(device):
        return {"frame": device // strips, "row": device % strips}

    barrier = pltpu.get_barrier_semaphore()

    def greet(j, carry):
        pl.semaphore_signal(
            barrier, inc=1, device_id=place((flat + j) % all_devices), device_id_type=MESH
        )
        return carry

    lax.fori_loop(1, all_devices, greet, 0)

    def arrived(ref, sem):
        pltpu.make_async_copy(ref, ref, sem).wait()

    def weight_copies(level):
        sources = (
            (w_ref.at[level, :, 0 : 2 * BLOCK, :], w_mid.at[level]),
            (w_ref.at[level, :, 2 * BLOCK : 2 * BLOCK + LANES, 0:LANES],
             w_first.at[level, :, 0:LANES, 0:LANES]),
            (w_ref.at[level, :, LANES : 2 * LANES, LANES:BLOCK],
             w_first.at[level, :, 0:LANES, LANES:BLOCK]),
            (w_ref.at[level, :, 2 * LANES : 2 * BLOCK, :],
             w_first.at[level, :, LANES : LANES + BLOCK, :]),
            (w_ref.at[level, :, 2 * BLOCK : 2 * BLOCK + LANES, LANES:BLOCK],
             w_last.at[level, :, BLOCK : BLOCK + LANES, LANES:BLOCK]),
            (w_ref.at[level, :, BLOCK : BLOCK + LANES, 0:LANES],
             w_last.at[level, :, BLOCK : BLOCK + LANES, 0:LANES]),
            (w_ref.at[level, :, 0:BLOCK, :], w_last.at[level, :, 0:BLOCK, :]),
        )
        return [
            pltpu.make_async_copy(source, target, w_sem.at[level, kind])
            for (source, target), kind in zip(sources, (0, 1, 1, 1, 2, 2, 2))
        ]

    def await_weights(level):
        for kind, w in enumerate((w_mid, w_first, w_last)):
            arrived(w.at[level], w_sem.at[level, kind])

    def fetch(n, p):
        return pltpu.make_async_copy(x_ref.at[n, :, p, :], planes.at[n, p], x_sem.at[n])

    def start_fetch(n):
        for p in range(phases):
            fetch(n, p).start()

    def edge(n, p, side):
        source = pl.ds(inner - MARGIN, MARGIN) if side == 0 else pl.ds(0, MARGIN)
        target = pl.ds(MARGIN, MARGIN) if side == 0 else pl.ds(0, MARGIN)
        return pltpu.make_async_remote_copy(
            src_ref=x_ref.at[n, source, p, :],
            dst_ref=edges.at[n, p, target, :],
            send_sem=e_send.at[side],
            recv_sem=e_recv.at[side, n],
            device_id={"row": row + 1 if side == 0 else row - 1},
            device_id_type=MESH,
        )

    for copy in weight_copies(0):
        copy.start()
    start_fetch(0)
    for level in range(1, SLEVELS):
        for copy in weight_copies(level):
            copy.start()
    for n in (2, 1, 3):
        start_fetch(n)

    pl.semaphore_wait(barrier, all_devices - 1)

    def start_edges(side):
        def one(n, carry):
            for p in range(phases):
                edge(n, p, side).start()
            return carry
        lax.fori_loop(0, frames, one, 0)

    @pl.when(jnp.logical_not(at_bottom))
    def _():
        start_edges(0)

    @pl.when(jnp.logical_not(at_top))
    def _():
        start_edges(1)

    def part_of(device):
        return pl.ds(pl.multiple_of((device % GROUP) * part, 8), part)

    def spot(device, n):
        return (device % GROUP) * frames + n

    def forward(n, c, k):
        peer = peers[k]
        return pltpu.make_async_remote_copy(
            src_ref=planes.at[n, c, part_of(peer), :],
            dst_ref=held.at[spot(me, n), c],
            send_sem=f_send.at[k],
            recv_sem=f_recv.at[c],
            device_id={"frame": peer},
            device_id_type=MESH,
        )

    def forward_own(n, c):
        return pltpu.make_async_copy(
            planes.at[n, c, part_of(me), :], held.at[spot(me, n), c], f_own.at[c]
        )

    def halo(c, side):
        return pltpu.make_async_remote_copy(
            src_ref=(to_before if side == 0 else to_after).at[c],
            dst_ref=(from_after if side == 0 else from_before).at[c],
            send_sem=h_send.at[side],
            recv_sem=h_recv.at[side, c],
            device_id={"frame": me - GROUP if side == 0 else me + GROUP},
            device_id_type=MESH,
        )

    def start_halos(c):
        @pl.when(jnp.logical_not(is_first))
        def _():
            halo(c, 0).start()

        @pl.when(jnp.logical_not(is_last))
        def _():
            halo(c, 1).start()

    def halo_arrivals(c):
        @pl.when(jnp.logical_not(is_last))
        def _():
            halo(c, 0).wait_recv()

        @pl.when(jnp.logical_not(is_first))
        def _():
            halo(c, 1).wait_recv()

    def back(i, c, k):
        peer = peers[k]
        return pltpu.make_async_remote_copy(
            src_ref=held.at[spot(peer, moved[i]), c],
            dst_ref=result.at[moved[i], c, part_of(me), :],
            send_sem=r_send.at[k],
            recv_sem=r_recv.at[k],
            device_id={"frame": peer},
            device_id_type=MESH,
        )

    def back_own(i, c):
        return pltpu.make_async_copy(
            held.at[spot(me, moved[i]), c], result.at[moved[i], c, part_of(me), :], r_own
        )

    def start_forward(n, c):
        for k in range(GROUP - 1):
            forward(n, c, k).start()
        forward_own(n, c).start()

    def split(rows, lanes, value):
        rounded = value.astype(jnp.bfloat16)
        high[rows, lanes] = rounded
        low[rows, lanes] = (value - rounded.astype(jnp.float32)).astype(jnp.bfloat16)

    everything = pl.ds(0, width)
    tile = 16

    def one_frame(step, carry):
        n = (2 * step) % 3 + 3 * (step // 3)
        arrived(planes.at[n], x_sem.at[n])

        def take(p, carry):
            for r in range(0, inner, tile):
                rows = pl.ds(pl.multiple_of(p * groups + r, tile), tile)
                split(rows, everything, planes[n, p, pl.ds(r, tile), :])
            return carry

        lax.fori_loop(0, phases, take, 0)

        @pl.when(jnp.logical_not(at_top))
        def _():
            arrived(edges.at[n, :, pl.ds(MARGIN, MARGIN), :], e_recv.at[0, n])

        @pl.when(jnp.logical_not(at_bottom))
        def _():
            arrived(edges.at[n, :, pl.ds(0, MARGIN), :], e_recv.at[1, n])

        def take_edges(p, carry):
            rows = pl.ds(pl.multiple_of(p * groups + inner, tile), tile)
            split(rows, everything, edges[n, p])
            return carry

        lax.fori_loop(0, phases, take_edges, 0)

        for level in range(SLEVELS):
            s = 2**level
            height = groups * (phases // s)

            @pl.when(step == 0)
            def _(level=level):
                await_weights(level)

            for b in range(width // BLOCK):
                if b == 0:
                    w, start, depth = w_first, 0, BLOCK + LANES
                elif b == width // BLOCK - 1:
                    w, start, depth = w_last, width - BLOCK - LANES, BLOCK + LANES
                else:
                    w, start, depth = w_mid, b * BLOCK - LANES, 2 * BLOCK
                xh = high[0:height, start : start + depth]
                xl = low[0:height, start : start + depth]
                wh, wl = w[level, 0], w[level, 1]
                buf[0:height, b * BLOCK : (b + 1) * BLOCK] = jnp.dot(
                    jnp.concatenate([xh, xl, xh], axis=1),
                    jnp.concatenate([wh, wh, wl], axis=0),
                    preferred_element_type=jnp.float32,
                )

            def rows(i, carry, level=level, s=s):
                lanes = pl.ds(pl.multiple_of(i * LANES, LANES), LANES)
                lane = lax.broadcasted_iota(jnp.int32, (1, LANES), 1)
                on = lane % s == 0
                x = {
                    p: buf[pl.ds(groups * (p // s), groups), lanes] for p in range(0, phases, s)
                }
                index = lax.broadcasted_iota(jnp.int32, (groups, LANES), 0)
                first = jnp.logical_and(index == 0, at_top)
                last = jnp.logical_and(index == inner - 1, at_bottom)
                for number, factor in enumerate(STEPS):
                    c = jnp.where(on, factor, 0.0)
                    if number % 2 == 0:
                        for p in range(s, phases, 2 * s):
                            if p + s < phases:
                                after = x[p + s]
                            else:
                                after = jnp.where(last, x[p - s], pltpu.roll(x[0], groups - 1, 0))
                            x[p] = x[p] + c * (x[p - s] + after)
                    else:
                        for p in range(0, phases, 2 * s):
                            if p > 0:
                                before = x[p - s]
                            else:
                                before = jnp.where(first, x[s], pltpu.roll(x[phases - s], 1, 0))
                            x[p] = x[p] + c * (before + x[p + s])
                up = jnp.where(on, LIFT_ZETA, 1.0)
                down = jnp.where(on, 1.0 / LIFT_ZETA, 1.0)
                for p in x:
                    is_low = p % (2 * s) == 0
                    value = x[p] * (up if is_low else down)
                    if is_low and level < SLEVELS - 1:
                        split(pl.ds(groups * (p // (2 * s)), groups), lanes, value)
                    else:
                        planes[n, p, :, lanes] = value[:inner]
                return carry

            lax.fori_loop(0, width // LANES, rows, 0)

            done = [
                p for p in range(0, phases, s) if p % (2 * s) != 0 or level == SLEVELS - 1
            ]

            @pl.when(step != 2)
            def _(done=done):
                for c in done:
                    start_forward(n, c)

        @pl.when(step == 2)
        def _():
            def high_frame(q, carry):
                c = phase_at(q)
                high_part = planes[kept, c] - 0.5 * (planes[kept - 1, c] + planes[kept + 1, c])
                planes[kept, c] = high_part
                result[kept, c] = high_part
                start_forward(kept, c)
                return carry

            lax.fori_loop(0, phases, high_frame, 0)

        return carry

    lax.fori_loop(0, frames, one_frame, 0)
    total = GROUP * frames

    def send_halo(q):
        c = phase_at(q)
        arrived(held.at[pl.ds(0, total - frames), c], f_recv.at[c])
        arrived(held.at[pl.ds(0, frames), c], f_own.at[c])

        def strip(i, carry):
            lanes = pl.ds(pl.multiple_of(i * LANES, LANES), LANES)
            left, right = outgoing([held[n, c, :, lanes] for n in range(total)])
            for j in range(TLEVELS):
                to_before[c, j, :, lanes] = left[j]
                to_after[c, j, :, lanes] = right[j]
            return carry

        lax.fori_loop(0, width // LANES, strip, 0)
        start_halos(c)

    def finish(q):
        c = phase_at(q)
        halo_arrivals(c)

        def strip(i, carry):
            lanes = pl.ds(pl.multiple_of(i * LANES, LANES), LANES)
            f = [held[n, c, :, lanes] for n in range(total)]
            before = [from_before[c, j, :, lanes] for j in range(TLEVELS)]
            after = [from_after[c, j, :, lanes] for j in range(TLEVELS)]
            out = temporal(f, before, after, is_first, is_last)
            sums = [None] * (TLEVELS + 1)
            for n in range(total):
                if n % frames in moved:
                    held[n, c, :, lanes] = out[n]
                t = level_of(n % 2**TLEVELS, TLEVELS) - 1
                square = out[n] * out[n]
                sums[t] = square if sums[t] is None else sums[t] + square
            return tuple(
                carry[t] + jnp.sum(sums[t].reshape(part // 8, 8, LANES), axis=0)
                for t in range(TLEVELS + 1)
            )

        zero = jnp.zeros((8, LANES), jnp.float32)
        sums = lax.fori_loop(0, width // LANES, strip, (zero,) * (TLEVELS + 1))
        for t in range(TLEVELS + 1):
            acc[c, t] = sums[t]
        for i in range(len(moved)):
            for k in range(GROUP - 1):
                back(i, c, k).start()
            back_own(i, c).start()

    send_halo(0)

    def middle(q, carry):
        send_halo(q)
        finish(q - 1)
        return carry

    lax.fori_loop(1, phases, middle, 0)
    finish(phases - 1)

    lane = lax.broadcasted_iota(jnp.int32, (1, LANES), 1)
    packed[...] = jnp.zeros_like(packed)
    for t in range(TLEVELS + 1):
        line = jnp.zeros((1, LANES), jnp.float32)
        for u in range(1, SLEVELS + 2):
            mine = sum(acc[c, t] for c in range(phases) if level_of(c, SLEVELS) == u)
            mine = jnp.sum(mine, axis=0, keepdims=True)
            distance = PERIOD
            while distance < LANES:
                mine = mine + pltpu.roll(mine, distance, 1)
                distance = 2 * distance
            line = jnp.where(lane // (LANES // (SLEVELS + 1)) == u - 1, mine, line)
        packed[pl.ds(t, 1), :] = line

    def to_other(j):
        return pltpu.make_async_remote_copy(
            src_ref=packed,
            dst_ref=inbox.at[flat],
            send_sem=s_send,
            recv_sem=s_recv,
            device_id=place((flat + j) % all_devices),
            device_id_type=MESH,
        )

    def start_sums(j, carry):
        to_other(j).start()
        return carry

    lax.fori_loop(1, all_devices, start_sums, 0)
    inbox[flat] = packed[...]

    arrived(inbox.at[pl.ds(0, all_devices - 1)], s_recv)
    sums = lax.fori_loop(1, all_devices, lambda j, s: s + inbox[j], inbox[0])
    counted = float(count * frames * strips * inner * phases * width)
    band, share = energy_tables(counted)
    energy[...] = share * jnp.dot(
        sums, band, precision=lax.Precision.HIGHEST, preferred_element_type=jnp.float32
    )

    for k in range(GROUP - 1):
        arrived(held.at[pl.ds(0, frames)], f_send.at[k])
        arrived(held.at[pl.ds(0, len(moved))], r_send.at[k])
        arrived(held.at[pl.ds(0, len(moved))], r_recv.at[k])
    arrived(held.at[pl.ds(0, len(moved))], r_own)
    arrived(inbox.at[pl.ds(0, all_devices - 1)], s_send)

    @pl.when(jnp.logical_not(is_first))
    def _():
        arrived(to_before, h_send.at[0])

    @pl.when(jnp.logical_not(is_last))
    def _():
        arrived(to_after, h_send.at[1])

    @pl.when(jnp.logical_not(at_bottom))
    def _():
        arrived(edges.at[:, :, pl.ds(MARGIN, MARGIN), :], e_send.at[0])

    @pl.when(jnp.logical_not(at_top))
    def _():
        arrived(edges.at[:, :, pl.ds(0, MARGIN), :], e_send.at[1])


def weave_kernel(planes, energy, o_ref, e_ref, sem):
    frames, phases = planes.shape[:2]
    for n in range(frames):
        for p in range(phases):
            pltpu.make_async_copy(planes.at[n, p], o_ref.at[n, :, p, :], sem).start()
    e_ref[...] = energy[: TLEVELS + 1, : 3 * SLEVELS + 1]
    pltpu.make_async_copy(planes, planes, sem).wait()


def shards(footage):
    frames, rows, width = footage.shape
    inner = rows // PERIOD
    groups = inner + 2 * MARGIN
    part = inner // GROUP
    strips = lax.axis_size("row")
    devices = lax.axis_size("frame") * strips
    any_space = pl.BlockSpec(memory_space=pl.ANY)
    vmem = pl.BlockSpec(memory_space=pltpu.VMEM)
    f32, bf16 = jnp.float32, jnp.bfloat16
    halo_buffer = pltpu.VMEM((PERIOD, TLEVELS, part, width), f32)
    dma = pltpu.SemaphoreType.DMA
    planes, energy = pl.pallas_call(
        video_kernel,
        out_shape=(
            jax.ShapeDtypeStruct((frames, PERIOD, inner, width), f32),
            jax.ShapeDtypeStruct((8, LANES), f32),
        ),
        in_specs=[any_space, pl.BlockSpec(memory_space=pltpu.HBM)],
        out_specs=(vmem, vmem),
        scratch_shapes=[
            pltpu.VMEM((frames, PERIOD, inner, width), f32),
            pltpu.VMEM((frames, PERIOD, 2 * MARGIN, width), f32),
            pltpu.VMEM((PERIOD * groups, width), bf16),
            pltpu.VMEM((PERIOD * groups, width), bf16),
            pltpu.VMEM((PERIOD * groups, width), f32),
            pltpu.VMEM((SLEVELS, 2, 2 * BLOCK, BLOCK), bf16),
            pltpu.VMEM((SLEVELS, 2, BLOCK + LANES, BLOCK), bf16),
            pltpu.VMEM((SLEVELS, 2, BLOCK + LANES, BLOCK), bf16),
            pltpu.VMEM((GROUP * frames, PERIOD, part, width), f32),
            halo_buffer, halo_buffer, halo_buffer, halo_buffer,
            pltpu.VMEM((PERIOD, TLEVELS + 1, 8, LANES), f32),
            pltpu.VMEM((8, LANES), f32),
            pltpu.VMEM((devices, 8, LANES), f32),
            dma((frames,)), dma((SLEVELS, 3)),
            dma((2,)), dma((2, frames)),
            dma((GROUP - 1,)), dma((PERIOD,)), dma((PERIOD,)),
            dma((2,)), dma((2, PERIOD)),
            dma((GROUP - 1,)), dma((GROUP - 1,)), dma,
            dma, dma,
        ],
        compiler_params=pltpu.CompilerParams(
            collective_id=0, has_side_effects=True, vmem_limit_bytes=40 * 2**20
        ),
    )(
        footage.reshape(frames, inner, PERIOD, width),
        jnp.asarray(column_weights(width)),
    )
    coeffs, means = pl.pallas_call(
        weave_kernel,
        out_shape=(
            jax.ShapeDtypeStruct((frames, inner, PERIOD, width), f32),
            jax.ShapeDtypeStruct((TLEVELS + 1, 3 * SLEVELS + 1), f32),
        ),
        in_specs=[vmem, vmem],
        out_specs=(any_space, vmem),
        scratch_shapes=[dma],
        compiler_params=pltpu.CompilerParams(vmem_limit_bytes=20 * 2**20),
    )(planes, energy)
    return coeffs.reshape(frames, rows, width), means


def solution(mesh):
    return jax.shard_map(
        shards,
        mesh=mesh,
        in_specs=(P("frame", "row", None),),
        out_specs=(P("frame", "row", None), P()),
        check_vma=False,
    )
```

```python
import jax
import jax.numpy as jnp
import numpy as np
from jax import lax
from jax.experimental import pallas as pl
from jax.experimental.pallas import tpu as pltpu
from jax.sharding import PartitionSpec as P

SLEVELS = 3
TLEVELS = 3
PERIOD = 2**SLEVELS
MARGIN = 8
GROUP = 4
PAIRED = 6
CUTS = 4
DIRECT = 1
BLOCK = 256
LANES = 128

LIFT_ALPHA = -1.586134342
LIFT_BETA = -0.05298011854
LIFT_GAMMA = 0.8829110762
LIFT_DELTA = 0.4435068522
LIFT_ZETA = 1.149604398
STEPS = (LIFT_ALPHA, LIFT_BETA, LIFT_GAMMA, LIFT_DELTA)
MESH = pl.DeviceIdType.MESH


def level_of(number, ceiling):
    depth_now = 1
    while number % 2 == 0 and depth_now <= ceiling:
        number = number // 2
        depth_now = depth_now + 1
    return depth_now


def space_band(row_level, col_level, levels):
    finest = min(row_level, col_level)
    if finest > levels:
        return 3 * levels
    if row_level == col_level:
        return 3 * (finest - 1) + 2
    if row_level == finest:
        return 3 * (finest - 1)
    return 3 * (finest - 1) + 1


def lifted_identity(size):
    x = np.eye(size)
    after = np.concatenate([np.arange(2, size, 2), [size - 2]])
    before = np.concatenate([[1], np.arange(1, size - 1, 2)])
    even, odd = np.arange(0, size, 2), np.arange(1, size, 2)
    x[:, odd] += LIFT_ALPHA * (x[:, even] + x[:, after])
    x[:, even] += LIFT_BETA * (x[:, before] + x[:, odd])
    x[:, odd] += LIFT_GAMMA * (x[:, even] + x[:, after])
    x[:, even] += LIFT_DELTA * (x[:, before] + x[:, odd])
    x[:, even] *= LIFT_ZETA
    x[:, odd] *= 1.0 / LIFT_ZETA
    return x


def high_and_low(x):
    x = np.asarray(x, np.float32)
    high = x.astype(jnp.bfloat16)
    return np.stack([high, (x - high.astype(np.float32)).astype(jnp.bfloat16)])


def column_weights(width):
    tables = []
    for level in range(SLEVELS):
        s = 2**level
        matrix = np.eye(width)
        matrix[::s, ::s] = lifted_identity(width // s)
        middle = matrix[LANES : LANES + 2 * BLOCK, BLOCK : 2 * BLOCK]
        first = matrix[:LANES, :LANES]
        last = matrix[width - LANES :, width - LANES :]
        tables.append(high_and_low(np.concatenate([middle, np.hstack([first, last])])))
    return np.stack(tables)


def energy_tables(counted):
    lane = lax.broadcasted_iota(jnp.int32, (LANES, LANES), 0)
    column = lax.broadcasted_iota(jnp.int32, (LANES, LANES), 1)
    u = lane // (LANES // (SLEVELS + 1)) + 1
    v = jnp.full_like(lane, 1)
    for level in range(1, SLEVELS + 1):
        v = v + jnp.where(lane % 2**level == 0, 1, 0)
    finest = jnp.minimum(u, v)
    kind = jnp.where(u == v, 2, jnp.where(u == finest, 0, 1))
    band = jnp.where(finest > SLEVELS, 3 * SLEVELS, 3 * (finest - 1) + kind)
    member = jnp.where(band == column, (SLEVELS + 1) * PERIOD / LANES, 0.0)
    t = lax.broadcasted_iota(jnp.int32, (8, LANES), 0)
    s = lax.broadcasted_iota(jnp.int32, (8, LANES), 1)
    share = jnp.full((8, LANES), 1.0 / counted, jnp.float32)
    for i in range(TLEVELS + 1):
        share = jnp.where(t == i, share * float(2 ** min(i + 1, TLEVELS)), share)
    for i in range(3 * SLEVELS + 1):
        share = jnp.where(s == i, share * float(4 ** min(i // 3 + 1, SLEVELS)), share)
    return member, share


def outgoing(f):
    o = {i: f[i] if i % 4 == 1 else f[i] - 0.5 * (f[i - 1] + f[i + 1]) for i in range(1, 14, 2)}
    a = {i: f[i] + 0.25 * (o[i - 1] + o[i + 1]) for i in range(2, 13, 2)}
    p6 = a[6] - 0.5 * (a[4] + a[8])
    p10 = a[10] - 0.5 * (a[8] + a[12])
    b8 = a[8] + 0.25 * (p6 + p10)
    to_before = (f[0], o[1], a[2] - 0.5 * a[4])
    to_after = (
        f[15] - 0.5 * f[14],
        f[14] + 0.25 * o[13] - 0.5 * a[12],
        a[12] + 0.25 * p10 - 0.5 * b8,
    )
    return to_before, to_after


def temporal(f, before, after, is_first, is_last):
    o = {i: f[i] if i % 4 == 1 else f[i] - 0.5 * (f[i - 1] + f[i + 1]) for i in range(1, 14, 2)}
    f16 = jnp.where(is_last, f[14], after[0])
    o[15] = f[15] - 0.5 * (f[14] + f16)
    o[-1] = jnp.where(is_first, o[1], before[0] - 0.5 * f[0])
    a = {i: f[i] + 0.25 * (o[i - 1] + o[i + 1]) for i in range(0, 16, 2)}
    a16 = jnp.where(is_last, a[12], after[0] + 0.25 * (o[15] + after[1]))
    a[16] = a16
    p = {i: a[i] - 0.5 * (a[i - 2] + a[i + 2]) for i in range(2, 16, 4)}
    p[-2] = jnp.where(is_first, p[2], before[1] + 0.25 * o[-1] - 0.5 * a[0])
    b = {i: a[i] + 0.25 * (p[i - 2] + p[i + 2]) for i in range(0, 16, 4)}
    b[16] = jnp.where(is_last, b[8], a16 + 0.25 * (p[14] + after[2] - 0.5 * a16))
    d4 = b[4] - 0.5 * (b[0] + b[8])
    d12 = b[12] - 0.5 * (b[8] + b[16])
    dm4 = jnp.where(is_first, d4, before[2] + 0.25 * p[-2] - 0.5 * b[0])
    out = {i: o[i] for i in range(1, 16, 2)}
    out.update({i: p[i] for i in range(2, 16, 4)})
    out[4], out[12] = d4, d12
    out[0] = b[0] + 0.25 * (dm4 + d4)
    out[8] = b[8] + 0.25 * (d4 + d12)
    return out


def phase_at(q):
    half, quarter = q // 4, (q // 2) % 2
    return (
        (1 - half) * (2 * q + 1)
        + half * (1 - quarter) * (4 * (q % 2) + 2)
        + half * quarter * 4 * (q % 2)
    )


def video_kernel(x_ref, w_ref, result, energy,
                 planes, edges, high, low, buf, w_mid, w_first, w_last,
                 near_in, far_in, made, held, from_before, from_after, to_before, to_after,
                 acc, packed, inbox, x_sem, w_sem, e_send, e_recv,
                 n_send, n_recv, p_send, p_recv, d_send,
                 f_send, f_recv, f_own, h_send, h_recv, r_send, r_recv, r_own, s_send, s_recv):
    frames, phases, inner, width = planes.shape
    groups = inner + 2 * MARGIN
    part = inner // GROUP
    cut = inner // CUTS
    chunks = PAIRED * CUTS
    straight = DIRECT * CUTS
    grouped = phases - PAIRED
    kept = 1
    moved = [n for n in range(frames) if n != kept]
    me = lax.axis_index("frame")
    row = lax.axis_index("row")
    strips = lax.axis_size("row")
    count = lax.axis_size("frame")
    at_top = row == 0
    at_bottom = row == strips - 1
    side = me % 2
    is_left = side == 0
    is_right = side == 1
    is_first = me // 2 == 0
    is_last = me // 2 == count // 2 - 1
    member = me % GROUP
    base = me - member
    starts = base == 0
    ends = base == count - GROUP
    peers = [base + (member + k) % GROUP for k in range(1, GROUP)]
    partner = me + 1 - 2 * side
    beyond = me - 2 + 4 * side

    all_devices = count * strips
    flat = me * strips + row

    def place(device):
        return {"frame": device // strips, "row": device % strips}

    barrier = pltpu.get_barrier_semaphore()

    def greet(j, carry):
        pl.semaphore_signal(
            barrier, inc=1, device_id=place((flat + j) % all_devices), device_id_type=MESH
        )
        return carry

    lax.fori_loop(1, all_devices, greet, 0)

    def arrived(ref, sem):
        pltpu.make_async_copy(ref, ref, sem).wait()

    def weight_copies(level):
        sources = (
            (w_ref.at[level, :, 0 : 2 * BLOCK, :], w_mid.at[level]),
            (w_ref.at[level, :, 2 * BLOCK : 2 * BLOCK + LANES, 0:LANES],
             w_first.at[level, :, 0:LANES, 0:LANES]),
            (w_ref.at[level, :, LANES : 2 * LANES, LANES:BLOCK],
             w_first.at[level, :, 0:LANES, LANES:BLOCK]),
            (w_ref.at[level, :, 2 * LANES : 2 * BLOCK, :],
             w_first.at[level, :, LANES : LANES + BLOCK, :]),
            (w_ref.at[level, :, 2 * BLOCK : 2 * BLOCK + LANES, LANES:BLOCK],
             w_last.at[level, :, BLOCK : BLOCK + LANES, LANES:BLOCK]),
            (w_ref.at[level, :, BLOCK : BLOCK + LANES, 0:LANES],
             w_last.at[level, :, BLOCK : BLOCK + LANES, 0:LANES]),
            (w_ref.at[level, :, 0:BLOCK, :], w_last.at[level, :, 0:BLOCK, :]),
        )
        return [
            pltpu.make_async_copy(source, target, w_sem.at[level, kind])
            for (source, target), kind in zip(sources, (0, 1, 1, 1, 2, 2, 2))
        ]

    def await_weights(level):
        for kind, w in enumerate((w_mid, w_first, w_last)):
            arrived(w.at[level], w_sem.at[level, kind])

    def fetch(n, p):
        return pltpu.make_async_copy(x_ref.at[n, :, p, :], planes.at[n, p], x_sem.at[n])

    def start_fetch(n):
        for p in range(phases):
            fetch(n, p).start()

    def edge(n, p, side):
        source = pl.ds(inner - MARGIN, MARGIN) if side == 0 else pl.ds(0, MARGIN)
        target = pl.ds(MARGIN, MARGIN) if side == 0 else pl.ds(0, MARGIN)
        return pltpu.make_async_remote_copy(
            src_ref=x_ref.at[n, source, p, :],
            dst_ref=edges.at[n, p, target, :],
            send_sem=e_send.at[side],
            recv_sem=e_recv.at[side, n],
            device_id={"row": row + 1 if side == 0 else row - 1},
            device_id_type=MESH,
        )

    for copy in weight_copies(0):
        copy.start()
    start_fetch(0)
    for level in range(1, SLEVELS):
        for copy in weight_copies(level):
            copy.start()
    for n in (2, 3, 1):
        start_fetch(n)

    pl.semaphore_wait(barrier, all_devices - 1)

    def start_edges(side):
        def one(n, carry):
            for p in range(phases):
                edge(n, p, side).start()
            return carry
        lax.fori_loop(0, frames, one, 0)

    @pl.when(jnp.logical_not(at_bottom))
    def _():
        start_edges(0)

    @pl.when(jnp.logical_not(at_top))
    def _():
        start_edges(1)

    def both(a, b):
        return jnp.logical_and(a, b)

    def no(a):
        return jnp.logical_not(a)

    def rows_of(i):
        return pl.ds(pl.multiple_of((i % CUTS) * cut, 8), cut)

    def spot(i):
        return phase_at(i // CUTS), rows_of(i)

    def slot(i):
        return i // CUTS, rows_of(i)

    def near(kind, i, source):
        return pltpu.make_async_remote_copy(
            src_ref=source,
            dst_ref=near_in.at[(kind,) + slot(i)],
            send_sem=n_send.at[kind],
            recv_sem=n_recv.at[kind, i],
            device_id={"frame": partner},
            device_id_type=MESH,
        )

    def far(kind, i, source):
        return pltpu.make_async_remote_copy(
            src_ref=source,
            dst_ref=far_in.at[(kind,) + slot(i)],
            send_sem=p_send.at[kind],
            recv_sem=p_recv.at[kind, i],
            device_id={"frame": beyond},
            device_id_type=MESH,
        )

    def direct(i, source):
        return pltpu.make_async_remote_copy(
            src_ref=source,
            dst_ref=near_in.at[(0,) + slot(i)],
            send_sem=d_send,
            recv_sem=n_recv.at[0, i],
            device_id={"frame": me - 1},
            device_id_type=MESH,
        )

    def take_near(kind, i):
        at = (kind,) + slot(i)
        arrived(near_in.at[at], n_recv.at[kind, i])
        return near_in[at]

    def await_far(kind, i):
        arrived(far_in.at[(kind,) + slot(i)], p_recv.at[kind, i])

    def take_far(kind, i):
        await_far(kind, i)
        return far_in[(kind,) + slot(i)]

    def relay(i, carry):
        await_far(0, i)
        near(0, i, far_in.at[(0,) + slot(i)]).start()
        return carry

    def relay_some(start, stop):
        @pl.when(both(is_left, no(is_last)))
        def _():
            lax.fori_loop(start, stop, relay, 0)

    def part_of(device):
        return pl.ds(pl.multiple_of((device % GROUP) * part, 8), part)

    def seat(device, n):
        return (device % GROUP) * frames + n

    def forward(n, g, k):
        peer = peers[k]
        return pltpu.make_async_remote_copy(
            src_ref=planes.at[n, phase_at(PAIRED + g), part_of(peer), :],
            dst_ref=held.at[seat(me, n), g],
            send_sem=f_send.at[k],
            recv_sem=f_recv.at[g],
            device_id={"frame": peer},
            device_id_type=MESH,
        )

    def forward_own(n, g):
        return pltpu.make_async_copy(
            planes.at[n, phase_at(PAIRED + g), part_of(me), :],
            held.at[seat(me, n), g],
            f_own.at[g],
        )

    def halo(c, side):
        return pltpu.make_async_remote_copy(
            src_ref=(to_before if side == 0 else to_after).at[c],
            dst_ref=(from_after if side == 0 else from_before).at[c],
            send_sem=h_send.at[side],
            recv_sem=h_recv.at[side, c],
            device_id={"frame": me - GROUP if side == 0 else me + GROUP},
            device_id_type=MESH,
        )

    def start_halos(c):
        @pl.when(jnp.logical_not(starts))
        def _():
            halo(c, 0).start()

        @pl.when(jnp.logical_not(ends))
        def _():
            halo(c, 1).start()

    def halo_arrivals(c):
        @pl.when(jnp.logical_not(ends))
        def _():
            halo(c, 0).wait_recv()

        @pl.when(jnp.logical_not(starts))
        def _():
            halo(c, 1).wait_recv()

    def back(i, c, k):
        peer = peers[k]
        return pltpu.make_async_remote_copy(
            src_ref=held.at[seat(peer, moved[i]), c],
            dst_ref=result.at[moved[i], phase_at(PAIRED + c), part_of(me), :],
            send_sem=r_send.at[k],
            recv_sem=r_recv.at[k],
            device_id={"frame": peer},
            device_id_type=MESH,
        )

    def back_own(i, c):
        return pltpu.make_async_copy(
            held.at[seat(me, moved[i]), c],
            result.at[moved[i], phase_at(PAIRED + c), part_of(me), :],
            r_own,
        )

    def start_forward(n, c):
        for k in range(GROUP - 1):
            forward(n, c, k).start()
        forward_own(n, c).start()

    def split(rows, lanes, value):
        rounded = value.astype(jnp.bfloat16)
        high[rows, lanes] = rounded
        low[rows, lanes] = (value - rounded.astype(jnp.float32)).astype(jnp.bfloat16)

    everything = pl.ds(0, width)
    tile = 16

    def one_frame(step, carry):
        n = (2 * step) % 5 - (step // 2) * (1 - step % 2)
        arrived(planes.at[n], x_sem.at[n])

        def take(p, carry):
            for r in range(0, inner, tile):
                rows = pl.ds(pl.multiple_of(p * groups + r, tile), tile)
                split(rows, everything, planes[n, p, pl.ds(r, tile), :])
            return carry

        lax.fori_loop(0, phases, take, 0)

        @pl.when(jnp.logical_not(at_top))
        def _():
            arrived(edges.at[n, :, pl.ds(MARGIN, MARGIN), :], e_recv.at[0, n])

        @pl.when(jnp.logical_not(at_bottom))
        def _():
            arrived(edges.at[n, :, pl.ds(0, MARGIN), :], e_recv.at[1, n])

        def take_edges(p, carry):
            rows = pl.ds(pl.multiple_of(p * groups + inner, tile), tile)
            split(rows, everything, edges[n, p])
            return carry

        lax.fori_loop(0, phases, take_edges, 0)

        for level in range(SLEVELS):
            s = 2**level
            height = groups * (phases // s)

            @pl.when(step == 0)
            def _(level=level):
                await_weights(level)

            for b in range(width // BLOCK):
                if b == 0:
                    w, start, depth = w_first, 0, BLOCK + LANES
                elif b == width // BLOCK - 1:
                    w, start, depth = w_last, width - BLOCK - LANES, BLOCK + LANES
                else:
                    w, start, depth = w_mid, b * BLOCK - LANES, 2 * BLOCK
                xh = high[0:height, start : start + depth]
                xl = low[0:height, start : start + depth]
                wh, wl = w[level, 0], w[level, 1]
                buf[0:height, b * BLOCK : (b + 1) * BLOCK] = jnp.dot(
                    jnp.concatenate([xh, xl, xh], axis=1),
                    jnp.concatenate([wh, wh, wl], axis=0),
                    preferred_element_type=jnp.float32,
                )

            def rows(i, carry, level=level, s=s):
                lanes = pl.ds(pl.multiple_of(i * LANES, LANES), LANES)
                lane = lax.broadcasted_iota(jnp.int32, (1, LANES), 1)
                on = lane % s == 0
                x = {
                    p: buf[pl.ds(groups * (p // s), groups), lanes] for p in range(0, phases, s)
                }
                index = lax.broadcasted_iota(jnp.int32, (groups, LANES), 0)
                first = jnp.logical_and(index == 0, at_top)
                last = jnp.logical_and(index == inner - 1, at_bottom)
                for number, factor in enumerate(STEPS):
                    c = jnp.where(on, factor, 0.0)
                    if number % 2 == 0:
                        for p in range(s, phases, 2 * s):
                            if p + s < phases:
                                after = x[p + s]
                            else:
                                after = jnp.where(last, x[p - s], pltpu.roll(x[0], groups - 1, 0))
                            x[p] = x[p] + c * (x[p - s] + after)
                    else:
                        for p in range(0, phases, 2 * s):
                            if p > 0:
                                before = x[p - s]
                            else:
                                before = jnp.where(first, x[s], pltpu.roll(x[phases - s], 1, 0))
                            x[p] = x[p] + c * (before + x[p + s])
                up = jnp.where(on, LIFT_ZETA, 1.0)
                down = jnp.where(on, 1.0 / LIFT_ZETA, 1.0)
                for p in x:
                    is_low = p % (2 * s) == 0
                    value = x[p] * (up if is_low else down)
                    if is_low and level < SLEVELS - 1:
                        split(pl.ds(groups * (p // (2 * s)), groups), lanes, value)
                    else:
                        planes[n, p, :, lanes] = value[:inner]
                return carry

            lax.fori_loop(0, width // LANES, rows, 0)

            done = [
                p for p in range(0, phases, s) if p % (2 * s) != 0 or level == SLEVELS - 1
            ]

            order = [phase_at(q) for q in range(phases)]

            def first_frames(to_right, done=done):
                for c in done:
                    if order.index(c) < PAIRED:
                        for r in range(CUTS):
                            i = order.index(c) * CUTS + r
                            source = planes.at[(0,) + spot(i)]
                            if to_right:
                                near(0, i, source).start()
                            elif i < straight:
                                direct(i, source).start()
                            else:
                                far(0, i, source).start()

            @pl.when(both(step == 0, is_right))
            def _(first_frames=first_frames):
                first_frames(True)

            @pl.when(both(step == 0, both(is_left, no(is_first))))
            def _(first_frames=first_frames):
                first_frames(False)

            @pl.when(step != 3)
            def _(done=done):
                for c in done:
                    if order.index(c) >= PAIRED:
                        start_forward(n, order.index(c) - PAIRED)

        @pl.when(step == 2)
        def _():
            def last_frame(i, carry):
                at = (3,) + spot(i)
                planes[at] = planes[at] - 0.5 * planes[(2,) + spot(i)]

                @pl.when(both(is_right, no(is_last)))
                def _():
                    far(0, i, planes.at[(3,) + spot(i)]).start()

                return carry

            lax.fori_loop(0, chunks, last_frame, 0)

        @pl.when(step == 3)
        def _():
            def high_frame(i, carry):
                at = spot(i)
                f0 = planes[(0,) + at]
                o1 = planes[(kept,) + at] - 0.5 * (f0 + planes[(2,) + at])
                result[(kept,) + at] = o1
                planes[(kept,) + at] = f0 + 0.25 * o1

                @pl.when(both(is_left, no(is_first)))
                def _():
                    far(1, i, planes.at[(kept,) + spot(i)]).start()

                return carry

            lax.fori_loop(0, chunks, high_frame, 0)

            def high_group(g, carry):
                c = phase_at(PAIRED + g)
                o1 = planes[kept, c] - 0.5 * (planes[kept - 1, c] + planes[kept + 1, c])
                planes[kept, c] = o1
                result[kept, c] = o1
                start_forward(kept, g)
                return carry

            lax.fori_loop(0, grouped, high_group, 0)

        @pl.when(step == 1)
        def _():
            relay_some(straight, straight + 3)

        @pl.when(step == 2)
        def _():
            relay_some(straight + 3, straight + 8)

        return carry

    lax.fori_loop(0, frames, one_frame, 0)
    acc[...] = jnp.zeros_like(acc)

    total = GROUP * frames

    def send_halo(c):
        arrived(held.at[pl.ds(0, total - frames), c], f_recv.at[c])
        arrived(held.at[pl.ds(0, frames), c], f_own.at[c])

        def strip(i, carry):
            lanes = pl.ds(pl.multiple_of(i * LANES, LANES), LANES)
            left, right = outgoing([held[n, c, :, lanes] for n in range(total)])
            for j in range(TLEVELS):
                to_before[c, j, :, lanes] = left[j]
                to_after[c, j, :, lanes] = right[j]
            return carry

        lax.fori_loop(0, width // LANES, strip, 0)
        start_halos(c)

    def finish(c):
        halo_arrivals(c)

        def strip(i, carry):
            lanes = pl.ds(pl.multiple_of(i * LANES, LANES), LANES)
            f = [held[n, c, :, lanes] for n in range(total)]
            before = [from_before[c, j, :, lanes] for j in range(TLEVELS)]
            after = [from_after[c, j, :, lanes] for j in range(TLEVELS)]
            out = temporal(f, before, after, starts, ends)
            sums = [None] * (TLEVELS + 1)
            for n in range(total):
                if n % frames in moved:
                    held[n, c, :, lanes] = out[n]
                t = level_of(n % 2**TLEVELS, TLEVELS) - 1
                square = out[n] * out[n]
                sums[t] = square if sums[t] is None else sums[t] + square
            return tuple(
                carry[t] + jnp.sum(sums[t].reshape(part // 8, 8, LANES), axis=0)
                for t in range(TLEVELS + 1)
            )

        zero = jnp.zeros((8, LANES), jnp.float32)
        sums = lax.fori_loop(0, width // LANES, strip, (zero,) * (TLEVELS + 1))
        for t in range(TLEVELS + 1):
            acc[phase_at(PAIRED + c), t] = sums[t]
        for i in range(len(moved)):
            back_own(i, c).start()

    def give_back(c):
        for i in range(len(moved)):
            for k in range(GROUP - 1):
                back(i, c, k).start()

    def count_in(n, t, i):
        c, rows = spot(i)
        value = result[n, c, rows, :]
        square = value * value
        folded = sum(square[:, k : k + LANES] for k in range(0, width, LANES))
        acc[c, t] += jnp.sum(folded.reshape(cut // 8, 8, LANES), axis=0)

    def loop(start, stop, body):
        def step(i, carry):
            body(i)
            return carry

        lax.fori_loop(start, stop, step, 0)

    lag = 4

    def halves(i):
        at = spot(i)
        return planes[(2,) + at], result[(1,) + at], result[(3,) + at], planes[(1,) + at]

    def third(i, after):
        at = spot(i)
        result[(3,) + at] = planes[(3,) + at] - 0.5 * after

    @pl.when(is_left)
    def _():
        def highs(i):
            third(i, take_near(0, i))

        def relays(i):
            @pl.when(no(is_last))
            def _():
                relay(i, 0)

        def questions(i):
            o3 = result[(3,) + spot(i)]
            made[(1,) + slot(i)] = 0.25 * o3

            @pl.when(no(is_last))
            def _():
                made[(1,) + slot(i)] = 0.25 * result[(3,) + spot(i)] + take_far(1, i)

            near(1, i, made.at[(1,) + slot(i)]).start()

        ahead = straight + 12
        loop(straight + 8, ahead, relays)
        loop(0, chunks - ahead, lambda i: (relays(i + ahead), highs(i)))
        loop(chunks - ahead, chunks, highs)
        loop(0, chunks, questions)

    @pl.when(is_right)
    def _():
        def highs(i):
            at = spot(i)

            @pl.when(is_last)
            def _():
                third(i, planes[(2,) + at])

            @pl.when(no(is_last))
            def _():
                third(i, take_near(0, i))

        def answer_highs(i):
            made[(0,) + slot(i)] = planes[(1,) + spot(i)]

            @pl.when(no(is_first))
            def _():
                made[(0,) + slot(i)] = planes[(1,) + spot(i)] + 0.25 * take_far(0, i)

            near(1, i, made.at[(0,) + slot(i)]).start()

        def highs_and_answers(i):
            highs(i)
            answer_highs(i - lag)

        loop(0, lag, highs)
        loop(lag, chunks, highs_and_answers)
        loop(chunks - lag, chunks, answer_highs)

    loop(0, grouped, send_halo)

    def left_seconds(i):
        at = spot(i)
        f2, o1, o3, h = halves(i)
        start = jnp.where(is_first, 0.125 * o1, -0.0625 * planes[(0,) + at])
        p2 = f2 + 0.25 * (o1 + o3) - 0.5 * h - 0.125 * o3 - start
        p2 = p2 - 0.5 * take_near(1, i)
        result[(2,) + at] = p2
        made[(2,) + slot(i)] = h + 0.25 * p2

        @pl.when(no(is_first))
        def _():
            far(2, i, made.at[(2,) + slot(i)]).start()

    def right_seconds(i):
        at = spot(i)
        f2, o1, o3, h = halves(i)
        came = take_near(1, i)
        p2 = f2 + 0.25 * (o1 + o3)
        p2 = p2 - jnp.where(is_last, h + came, 0.5 * (h + came) + 0.125 * o3)
        result[(2,) + at] = p2
        made[(1,) + slot(i)] = 0.25 * (o3 + p2)

        @pl.when(no(is_last))
        def _():
            far(1, i, made.at[(1,) + slot(i)]).start()

    def seconds(j):
        @pl.when(is_left)
        def _():
            loop(j * CUTS, (j + 1) * CUTS, left_seconds)

        @pl.when(is_right)
        def _():
            loop(j * CUTS, (j + 1) * CUTS, right_seconds)

    loop(0, PAIRED, seconds)
    loop(0, grouped, finish)

    @pl.when(is_left)
    def _():
        def thirds(i):
            f2, o1, o3, h = halves(i)
            p2 = result[(2,) + spot(i)]
            own = 0.25 * (o3 + p2) - jnp.where(is_last, 1.0, 0.5) * made[(2,) + slot(i)]
            made[(3,) + slot(i)] = own - jnp.where(is_first, 0.125, 0.0) * (o1 + p2)

            @pl.when(no(is_last))
            def _():
                made[(3,) + slot(i)] -= 0.5 * take_far(2, i)

            near(2, i, made.at[(3,) + slot(i)]).start()

        loop(0, 0, give_back)
        loop(0, chunks, thirds)
        loop(0, grouped, give_back)

        def sums_so_far(i):
            count_in(1, 0, i)
            count_in(3, 0, i)
            count_in(2, 1, i)

        loop(0, chunks, sums_so_far)

        def lows(i):
            at = spot(i)
            start = jnp.where(is_first, 0.25, 0.0) * (result[(1,) + at] + result[(2,) + at])
            result[(0,) + at] = made[(2,) + slot(i)] + start + take_near(2, i)
            count_in(0, 3, i)

        loop(0, chunks, lows)

    @pl.when(is_right)
    def _():
        def thirds(i):
            at = spot(i)
            mine = made[(1,) + slot(i)]
            scale = jnp.where(is_last, 0.0, 0.5)
            result[(0,) + at] = (
                planes[(1,) + at] + 0.25 * result[(2,) + at] - scale * mine
            )

            @pl.when(no(is_first))
            def _():
                result[(0,) + at] -= jnp.where(is_last, 1.0, 0.5) * take_far(1, i)

            d = result[(0,) + at] + take_near(2, i)
            result[(0,) + at] = d
            made[(2,) + slot(i)] = mine + 0.25 * d

            @pl.when(no(is_last))
            def _():
                far(2, i, made.at[(2,) + slot(i)]).start()

        def answer_thirds(i):
            made[(3,) + slot(i)] = jnp.where(is_first, 0.5, 0.25) * result[(0,) + spot(i)]

            @pl.when(no(is_first))
            def _():
                made[(3,) + slot(i)] += take_far(2, i)

            near(2, i, made.at[(3,) + slot(i)]).start()

        def thirds_and_answers(i):
            thirds(i)
            answer_thirds(i - lag)

        loop(0, 1, give_back)
        loop(0, lag, thirds)
        loop(lag, chunks, thirds_and_answers)
        loop(chunks - lag, chunks, answer_thirds)
        loop(1, grouped, give_back)

        def all_sums(i):
            count_in(1, 0, i)
            count_in(3, 0, i)
            count_in(2, 1, i)
            count_in(0, 2, i)

        loop(0, chunks, all_sums)

    lane = lax.broadcasted_iota(jnp.int32, (1, LANES), 1)
    packed[...] = jnp.zeros_like(packed)
    for t in range(TLEVELS + 1):
        line = jnp.zeros((1, LANES), jnp.float32)
        for u in range(1, SLEVELS + 2):
            mine = sum(acc[c, t] for c in range(phases) if level_of(c, SLEVELS) == u)
            mine = jnp.sum(mine, axis=0, keepdims=True)
            distance = PERIOD
            while distance < LANES:
                mine = mine + pltpu.roll(mine, distance, 1)
                distance = 2 * distance
            line = jnp.where(lane // (LANES // (SLEVELS + 1)) == u - 1, mine, line)
        packed[pl.ds(t, 1), :] = line

    def to_other(j):
        return pltpu.make_async_remote_copy(
            src_ref=packed,
            dst_ref=inbox.at[flat],
            send_sem=s_send,
            recv_sem=s_recv,
            device_id=place((flat + j) % all_devices),
            device_id_type=MESH,
        )

    def start_sums(j, carry):
        to_other(j).start()
        return carry

    lax.fori_loop(1, all_devices, start_sums, 0)
    inbox[flat] = packed[...]

    arrived(inbox.at[pl.ds(0, all_devices - 1)], s_recv)
    sums = lax.fori_loop(1, all_devices, lambda j, s: s + inbox[j], inbox[0])
    counted = float(count * frames * strips * inner * phases * width)
    band, share = energy_tables(counted)
    energy[...] = share * jnp.dot(
        sums, band, precision=lax.Precision.HIGHEST, preferred_element_type=jnp.float32
    )

    arrived(inbox.at[pl.ds(0, all_devices - 1)], s_send)
    for k in range(GROUP - 1):
        arrived(held.at[pl.ds(0, frames)], f_send.at[k])
        arrived(held.at[pl.ds(0, len(moved))], r_send.at[k])
        arrived(held.at[pl.ds(0, len(moved))], r_recv.at[k])
    arrived(held.at[pl.ds(0, len(moved))], r_own)

    @pl.when(jnp.logical_not(starts))
    def _():
        arrived(to_before, h_send.at[0])

    @pl.when(jnp.logical_not(ends))
    def _():
        arrived(to_after, h_send.at[1])

    for kind in (1, 2):
        arrived(near_in.at[kind], n_send.at[kind])

    @pl.when(is_right)
    def _():
        arrived(near_in.at[0], n_send.at[0])

    @pl.when(both(is_left, no(is_last)))
    def _():
        arrived(near_in.at[0, pl.ds(0, PAIRED - DIRECT)], n_send.at[0])

    @pl.when(jnp.logical_or(both(is_left, no(is_first)), both(is_right, no(is_last))))
    def _():
        for kind in (1, 2):
            arrived(far_in.at[kind], p_send.at[kind])

    @pl.when(both(is_left, no(is_first)))
    def _():
        arrived(near_in.at[0, pl.ds(0, DIRECT)], d_send)
        arrived(far_in.at[0, pl.ds(0, PAIRED - DIRECT)], p_send.at[0])

    @pl.when(both(is_right, no(is_last)))
    def _():
        arrived(far_in.at[0], p_send.at[0])

    @pl.when(jnp.logical_not(at_bottom))
    def _():
        arrived(edges.at[:, :, pl.ds(MARGIN, MARGIN), :], e_send.at[0])

    @pl.when(jnp.logical_not(at_top))
    def _():
        arrived(edges.at[:, :, pl.ds(0, MARGIN), :], e_send.at[1])


def weave_kernel(planes, energy, o_ref, e_ref, sem):
    frames, phases = planes.shape[:2]
    for n in range(frames):
        for p in range(phases):
            pltpu.make_async_copy(planes.at[n, p], o_ref.at[n, :, p, :], sem).start()
    e_ref[...] = energy[: TLEVELS + 1, : 3 * SLEVELS + 1]
    pltpu.make_async_copy(planes, planes, sem).wait()


def shards(footage):
    frames, rows, width = footage.shape
    inner = rows // PERIOD
    groups = inner + 2 * MARGIN
    strips = lax.axis_size("row")
    devices = lax.axis_size("frame") * strips
    any_space = pl.BlockSpec(memory_space=pl.ANY)
    vmem = pl.BlockSpec(memory_space=pltpu.VMEM)
    f32, bf16 = jnp.float32, jnp.bfloat16
    traffic = pltpu.VMEM((3, PAIRED, inner, width), f32)
    chunks = PAIRED * CUTS
    grouped = PERIOD - PAIRED
    part = inner // GROUP
    halo_buffer = pltpu.VMEM((grouped, TLEVELS, part, width), f32)
    dma = pltpu.SemaphoreType.DMA
    planes, energy = pl.pallas_call(
        video_kernel,
        out_shape=(
            jax.ShapeDtypeStruct((frames, PERIOD, inner, width), f32),
            jax.ShapeDtypeStruct((8, LANES), f32),
        ),
        in_specs=[any_space, pl.BlockSpec(memory_space=pltpu.HBM)],
        out_specs=(vmem, vmem),
        scratch_shapes=[
            pltpu.VMEM((frames, PERIOD, inner, width), f32),
            pltpu.VMEM((frames, PERIOD, 2 * MARGIN, width), f32),
            pltpu.VMEM((PERIOD * groups, width), bf16),
            pltpu.VMEM((PERIOD * groups, width), bf16),
            pltpu.VMEM((PERIOD * groups, width), f32),
            pltpu.VMEM((SLEVELS, 2, 2 * BLOCK, BLOCK), bf16),
            pltpu.VMEM((SLEVELS, 2, BLOCK + LANES, BLOCK), bf16),
            pltpu.VMEM((SLEVELS, 2, BLOCK + LANES, BLOCK), bf16),
            traffic,
            traffic,
            pltpu.VMEM((4, PAIRED, inner, width), f32),
            pltpu.VMEM((GROUP * frames, grouped, part, width), f32),
            halo_buffer, halo_buffer, halo_buffer, halo_buffer,
            pltpu.VMEM((PERIOD, TLEVELS + 1, 8, LANES), f32),
            pltpu.VMEM((8, LANES), f32),
            pltpu.VMEM((devices, 8, LANES), f32),
            dma((frames,)), dma((SLEVELS, 3)),
            dma((2,)), dma((2, frames)),
            dma((3,)), dma((3, chunks)), dma((3,)), dma((3, chunks)), dma,
            dma((GROUP - 1,)), dma((grouped,)), dma((grouped,)),
            dma((2,)), dma((2, grouped)),
            dma((GROUP - 1,)), dma((GROUP - 1,)), dma,
            dma, dma,
        ],
        compiler_params=pltpu.CompilerParams(
            collective_id=0, has_side_effects=True, vmem_limit_bytes=44 * 2**20
        ),
    )(
        footage.reshape(frames, inner, PERIOD, width),
        jnp.asarray(column_weights(width)),
    )
    coeffs, means = pl.pallas_call(
        weave_kernel,
        out_shape=(
            jax.ShapeDtypeStruct((frames, inner, PERIOD, width), f32),
            jax.ShapeDtypeStruct((TLEVELS + 1, 3 * SLEVELS + 1), f32),
        ),
        in_specs=[vmem, vmem],
        out_specs=(any_space, vmem),
        scratch_shapes=[dma],
        compiler_params=pltpu.CompilerParams(vmem_limit_bytes=20 * 2**20),
    )(planes, energy)
    return coeffs.reshape(frames, rows, width), means


def solution(mesh):
    return jax.shard_map(
        shards,
        mesh=mesh,
        in_specs=(P("frame", "row", None),),
        out_specs=(P("frame", "row", None), P()),
        check_vma=False,
    )
```

```python
import jax
import jax.numpy as jnp
import numpy as np
from jax import lax
from jax.experimental import pallas as pl
from jax.experimental.pallas import tpu as pltpu
from jax.sharding import PartitionSpec as P

SLEVELS = 3
TLEVELS = 3
PERIOD = 2**SLEVELS
MARGIN = 8
GROUP = 4
PAIRED = 6
CUTS = 4
DIRECT = 1
BLOCK = 256
LANES = 128

LIFT_ALPHA = -1.586134342
LIFT_BETA = -0.05298011854
LIFT_GAMMA = 0.8829110762
LIFT_DELTA = 0.4435068522
LIFT_ZETA = 1.149604398
STEPS = (LIFT_ALPHA, LIFT_BETA, LIFT_GAMMA, LIFT_DELTA)
MESH = pl.DeviceIdType.MESH


def level_of(number, ceiling):
    depth_now = 1
    while number % 2 == 0 and depth_now <= ceiling:
        number = number // 2
        depth_now = depth_now + 1
    return depth_now


def space_band(row_level, col_level, levels):
    finest = min(row_level, col_level)
    if finest > levels:
        return 3 * levels
    if row_level == col_level:
        return 3 * (finest - 1) + 2
    if row_level == finest:
        return 3 * (finest - 1)
    return 3 * (finest - 1) + 1


def lifted_identity(size):
    x = np.eye(size)
    after = np.concatenate([np.arange(2, size, 2), [size - 2]])
    before = np.concatenate([[1], np.arange(1, size - 1, 2)])
    even, odd = np.arange(0, size, 2), np.arange(1, size, 2)
    x[:, odd] += LIFT_ALPHA * (x[:, even] + x[:, after])
    x[:, even] += LIFT_BETA * (x[:, before] + x[:, odd])
    x[:, odd] += LIFT_GAMMA * (x[:, even] + x[:, after])
    x[:, even] += LIFT_DELTA * (x[:, before] + x[:, odd])
    x[:, even] *= LIFT_ZETA
    x[:, odd] *= 1.0 / LIFT_ZETA
    return x


def high_and_low(x):
    x = np.asarray(x, np.float32)
    high = x.astype(jnp.bfloat16)
    return np.stack([high, (x - high.astype(np.float32)).astype(jnp.bfloat16)])


def column_weights(width):
    tables = []
    for level in range(SLEVELS):
        s = 2**level
        matrix = np.eye(width)
        matrix[::s, ::s] = lifted_identity(width // s)
        middle = matrix[LANES : LANES + 2 * BLOCK, BLOCK : 2 * BLOCK]
        first = matrix[:LANES, :LANES]
        last = matrix[width - LANES :, width - LANES :]
        tables.append(high_and_low(np.concatenate([middle, np.hstack([first, last])])))
    return np.stack(tables)


def energy_tables(counted):
    lane = lax.broadcasted_iota(jnp.int32, (LANES, LANES), 0)
    column = lax.broadcasted_iota(jnp.int32, (LANES, LANES), 1)
    u = lane // (LANES // (SLEVELS + 1)) + 1
    v = jnp.full_like(lane, 1)
    for level in range(1, SLEVELS + 1):
        v = v + jnp.where(lane % 2**level == 0, 1, 0)
    finest = jnp.minimum(u, v)
    kind = jnp.where(u == v, 2, jnp.where(u == finest, 0, 1))
    band = jnp.where(finest > SLEVELS, 3 * SLEVELS, 3 * (finest - 1) + kind)
    member = jnp.where(band == column, (SLEVELS + 1) * PERIOD / LANES, 0.0)
    t = lax.broadcasted_iota(jnp.int32, (8, LANES), 0)
    s = lax.broadcasted_iota(jnp.int32, (8, LANES), 1)
    share = jnp.full((8, LANES), 1.0 / counted, jnp.float32)
    for i in range(TLEVELS + 1):
        share = jnp.where(t == i, share * float(2 ** min(i + 1, TLEVELS)), share)
    for i in range(3 * SLEVELS + 1):
        share = jnp.where(s == i, share * float(4 ** min(i // 3 + 1, SLEVELS)), share)
    return member, share


def outgoing(f):
    o = {i: f[i] if i % 4 == 1 else f[i] - 0.5 * (f[i - 1] + f[i + 1]) for i in range(1, 14, 2)}
    a = {i: f[i] + 0.25 * (o[i - 1] + o[i + 1]) for i in range(2, 13, 2)}
    p6 = a[6] - 0.5 * (a[4] + a[8])
    p10 = a[10] - 0.5 * (a[8] + a[12])
    b8 = a[8] + 0.25 * (p6 + p10)
    to_before = (f[0], o[1], a[2] - 0.5 * a[4])
    to_after = (
        f[15] - 0.5 * f[14],
        f[14] + 0.25 * o[13] - 0.5 * a[12],
        a[12] + 0.25 * p10 - 0.5 * b8,
    )
    return to_before, to_after


def temporal(f, before, after, is_first, is_last):
    o = {i: f[i] if i % 4 == 1 else f[i] - 0.5 * (f[i - 1] + f[i + 1]) for i in range(1, 14, 2)}
    f16 = jnp.where(is_last, f[14], after[0])
    o[15] = f[15] - 0.5 * (f[14] + f16)
    o[-1] = jnp.where(is_first, o[1], before[0] - 0.5 * f[0])
    a = {i: f[i] + 0.25 * (o[i - 1] + o[i + 1]) for i in range(0, 16, 2)}
    a16 = jnp.where(is_last, a[12], after[0] + 0.25 * (o[15] + after[1]))
    a[16] = a16
    p = {i: a[i] - 0.5 * (a[i - 2] + a[i + 2]) for i in range(2, 16, 4)}
    p[-2] = jnp.where(is_first, p[2], before[1] + 0.25 * o[-1] - 0.5 * a[0])
    b = {i: a[i] + 0.25 * (p[i - 2] + p[i + 2]) for i in range(0, 16, 4)}
    b[16] = jnp.where(is_last, b[8], a16 + 0.25 * (p[14] + after[2] - 0.5 * a16))
    d4 = b[4] - 0.5 * (b[0] + b[8])
    d12 = b[12] - 0.5 * (b[8] + b[16])
    dm4 = jnp.where(is_first, d4, before[2] + 0.25 * p[-2] - 0.5 * b[0])
    out = {i: o[i] for i in range(1, 16, 2)}
    out.update({i: p[i] for i in range(2, 16, 4)})
    out[4], out[12] = d4, d12
    out[0] = b[0] + 0.25 * (dm4 + d4)
    out[8] = b[8] + 0.25 * (d4 + d12)
    return out


def phase_at(q):
    half, quarter = q // 4, (q // 2) % 2
    return (
        (1 - half) * (2 * q + 1)
        + half * (1 - quarter) * (4 * (q % 2) + 2)
        + half * quarter * 4 * (q % 2)
    )


def video_kernel(x_ref, w_ref, result, energy,
                 planes, edges, high, low, buf, w_mid, w_first, w_last,
                 near_in, far_in, made, held, from_before, from_after, to_before, to_after,
                 acc, packed, inbox, x_sem, w_sem, e_send, e_recv,
                 n_send, n_recv, p_send, p_recv, d_send,
                 f_send, f_recv, f_own, h_send, h_recv, r_send, r_recv, r_own, s_send, s_recv):
    frames, phases, inner, width = planes.shape
    groups = inner + 2 * MARGIN
    part = inner // GROUP
    cut = inner // CUTS
    chunks = PAIRED * CUTS
    straight = DIRECT * CUTS
    grouped = phases - PAIRED
    kept = 1
    moved = [n for n in range(frames) if n != kept]
    me = lax.axis_index("frame")
    row = lax.axis_index("row")
    strips = lax.axis_size("row")
    count = lax.axis_size("frame")
    at_top = row == 0
    at_bottom = row == strips - 1
    side = me % 2
    is_left = side == 0
    is_right = side == 1
    is_first = me // 2 == 0
    is_last = me // 2 == count // 2 - 1
    member = me % GROUP
    base = me - member
    starts = base == 0
    ends = base == count - GROUP
    peers = [base + (member + k) % GROUP for k in range(1, GROUP)]
    partner = me + 1 - 2 * side
    beyond = me - 2 + 4 * side

    all_devices = count * strips
    flat = me * strips + row

    def place(device):
        return {"frame": device // strips, "row": device % strips}

    barrier = pltpu.get_barrier_semaphore()

    def greet(j, carry):
        pl.semaphore_signal(
            barrier, inc=1, device_id=place((flat + j) % all_devices), device_id_type=MESH
        )
        return carry

    lax.fori_loop(1, all_devices, greet, 0)

    def arrived(ref, sem):
        pltpu.make_async_copy(ref, ref, sem).wait()

    def weight_copies(level):
        sources = (
            (w_ref.at[level, :, 0 : 2 * BLOCK, :], w_mid.at[level]),
            (w_ref.at[level, :, 2 * BLOCK : 2 * BLOCK + LANES, 0:LANES],
             w_first.at[level, :, 0:LANES, 0:LANES]),
            (w_ref.at[level, :, LANES : 2 * LANES, LANES:BLOCK],
             w_first.at[level, :, 0:LANES, LANES:BLOCK]),
            (w_ref.at[level, :, 2 * LANES : 2 * BLOCK, :],
             w_first.at[level, :, LANES : LANES + BLOCK, :]),
            (w_ref.at[level, :, 2 * BLOCK : 2 * BLOCK + LANES, LANES:BLOCK],
             w_last.at[level, :, BLOCK : BLOCK + LANES, LANES:BLOCK]),
            (w_ref.at[level, :, BLOCK : BLOCK + LANES, 0:LANES],
             w_last.at[level, :, BLOCK : BLOCK + LANES, 0:LANES]),
            (w_ref.at[level, :, 0:BLOCK, :], w_last.at[level, :, 0:BLOCK, :]),
        )
        return [
            pltpu.make_async_copy(source, target, w_sem.at[level, kind])
            for (source, target), kind in zip(sources, (0, 1, 1, 1, 2, 2, 2))
        ]

    def await_weights(level):
        for kind, w in enumerate((w_mid, w_first, w_last)):
            arrived(w.at[level], w_sem.at[level, kind])

    def fetch(n, p):
        return pltpu.make_async_copy(x_ref.at[n, :, p, :], planes.at[n, p], x_sem.at[n])

    def start_fetch(n):
        for p in range(phases):
            fetch(n, p).start()

    def edge(n, p, side):
        source = pl.ds(inner - MARGIN, MARGIN) if side == 0 else pl.ds(0, MARGIN)
        target = pl.ds(MARGIN, MARGIN) if side == 0 else pl.ds(0, MARGIN)
        return pltpu.make_async_remote_copy(
            src_ref=x_ref.at[n, source, p, :],
            dst_ref=edges.at[n, p, target, :],
            send_sem=e_send.at[side],
            recv_sem=e_recv.at[side, n],
            device_id={"row": row + 1 if side == 0 else row - 1},
            device_id_type=MESH,
        )

    for copy in weight_copies(0):
        copy.start()
    start_fetch(0)
    for level in range(1, SLEVELS):
        for copy in weight_copies(level):
            copy.start()
    for n in (2, 3, 1):
        start_fetch(n)

    pl.semaphore_wait(barrier, all_devices - 1)

    def start_edges(side):
        def one(n, carry):
            for p in range(phases):
                edge(n, p, side).start()
            return carry
        lax.fori_loop(0, frames, one, 0)

    @pl.when(jnp.logical_not(at_bottom))
    def _():
        start_edges(0)

    @pl.when(jnp.logical_not(at_top))
    def _():
        start_edges(1)

    def both(a, b):
        return jnp.logical_and(a, b)

    def no(a):
        return jnp.logical_not(a)

    def rows_of(i):
        return pl.ds(pl.multiple_of((i % CUTS) * cut, 8), cut)

    def spot(i):
        return phase_at(i // CUTS), rows_of(i)

    def slot(i):
        return i // CUTS, rows_of(i)

    def near(kind, i, source):
        return pltpu.make_async_remote_copy(
            src_ref=source,
            dst_ref=near_in.at[(kind,) + slot(i)],
            send_sem=n_send.at[kind],
            recv_sem=n_recv.at[kind, i],
            device_id={"frame": partner},
            device_id_type=MESH,
        )

    def far(kind, i, source):
        return pltpu.make_async_remote_copy(
            src_ref=source,
            dst_ref=far_in.at[(kind,) + slot(i)],
            send_sem=p_send.at[kind],
            recv_sem=p_recv.at[kind, i],
            device_id={"frame": beyond},
            device_id_type=MESH,
        )

    def direct(i, source):
        return pltpu.make_async_remote_copy(
            src_ref=source,
            dst_ref=near_in.at[(0,) + slot(i)],
            send_sem=d_send,
            recv_sem=n_recv.at[0, i],
            device_id={"frame": me - 1},
            device_id_type=MESH,
        )

    def take_near(kind, i):
        at = (kind,) + slot(i)
        arrived(near_in.at[at], n_recv.at[kind, i])
        return near_in[at]

    def await_far(kind, i):
        arrived(far_in.at[(kind,) + slot(i)], p_recv.at[kind, i])

    def take_far(kind, i):
        await_far(kind, i)
        return far_in[(kind,) + slot(i)]

    def relay(i, carry):
        await_far(0, i)
        near(0, i, far_in.at[(0,) + slot(i)]).start()
        return carry

    def relay_some(start, stop):
        @pl.when(both(is_left, no(is_last)))
        def _():
            lax.fori_loop(start, stop, relay, 0)

    def part_of(device):
        return pl.ds(pl.multiple_of((device % GROUP) * part, 8), part)

    def seat(device, n):
        return (device % GROUP) * frames + n

    def forward(n, g, k):
        peer = peers[k]
        return pltpu.make_async_remote_copy(
            src_ref=planes.at[n, phase_at(PAIRED + g), part_of(peer), :],
            dst_ref=held.at[seat(me, n), g],
            send_sem=f_send.at[k],
            recv_sem=f_recv.at[g],
            device_id={"frame": peer},
            device_id_type=MESH,
        )

    def forward_own(n, g):
        return pltpu.make_async_copy(
            planes.at[n, phase_at(PAIRED + g), part_of(me), :],
            held.at[seat(me, n), g],
            f_own.at[g],
        )

    def halo(c, side):
        return pltpu.make_async_remote_copy(
            src_ref=(to_before if side == 0 else to_after).at[c],
            dst_ref=(from_after if side == 0 else from_before).at[c],
            send_sem=h_send.at[side],
            recv_sem=h_recv.at[side, c],
            device_id={"frame": me - GROUP if side == 0 else me + GROUP},
            device_id_type=MESH,
        )

    def start_halos(c):
        @pl.when(jnp.logical_not(starts))
        def _():
            halo(c, 0).start()

        @pl.when(jnp.logical_not(ends))
        def _():
            halo(c, 1).start()

    def halo_arrivals(c):
        @pl.when(jnp.logical_not(ends))
        def _():
            halo(c, 0).wait_recv()

        @pl.when(jnp.logical_not(starts))
        def _():
            halo(c, 1).wait_recv()

    def back(i, c, k):
        peer = peers[k]
        return pltpu.make_async_remote_copy(
            src_ref=held.at[seat(peer, moved[i]), c],
            dst_ref=result.at[moved[i], phase_at(PAIRED + c), part_of(me), :],
            send_sem=r_send.at[k],
            recv_sem=r_recv.at[k],
            device_id={"frame": peer},
            device_id_type=MESH,
        )

    def back_own(i, c):
        return pltpu.make_async_copy(
            held.at[seat(me, moved[i]), c],
            result.at[moved[i], phase_at(PAIRED + c), part_of(me), :],
            r_own,
        )

    def start_forward(n, c):
        for k in range(GROUP - 1):
            forward(n, c, k).start()
        forward_own(n, c).start()

    def split(rows, lanes, value):
        rounded = value.astype(jnp.bfloat16)
        high[rows, lanes] = rounded
        low[rows, lanes] = (value - rounded.astype(jnp.float32)).astype(jnp.bfloat16)

    everything = pl.ds(0, width)
    tile = 16

    def one_frame(step, carry):
        n = (2 * step) % 5 - (step // 2) * (1 - step % 2)
        arrived(planes.at[n], x_sem.at[n])

        def take(p, carry):
            for r in range(0, inner, tile):
                rows = pl.ds(pl.multiple_of(p * groups + r, tile), tile)
                split(rows, everything, planes[n, p, pl.ds(r, tile), :])
            return carry

        lax.fori_loop(0, phases, take, 0)

        @pl.when(jnp.logical_not(at_top))
        def _():
            arrived(edges.at[n, :, pl.ds(MARGIN, MARGIN), :], e_recv.at[0, n])

        @pl.when(jnp.logical_not(at_bottom))
        def _():
            arrived(edges.at[n, :, pl.ds(0, MARGIN), :], e_recv.at[1, n])

        def take_edges(p, carry):
            rows = pl.ds(pl.multiple_of(p * groups + inner, tile), tile)
            split(rows, everything, edges[n, p])
            return carry

        lax.fori_loop(0, phases, take_edges, 0)

        for level in range(SLEVELS):
            s = 2**level
            height = groups * (phases // s)

            @pl.when(step == 0)
            def _(level=level):
                await_weights(level)

            for b in range(width // BLOCK):
                if b == 0:
                    w, start, depth = w_first, 0, BLOCK + LANES
                elif b == width // BLOCK - 1:
                    w, start, depth = w_last, width - BLOCK - LANES, BLOCK + LANES
                else:
                    w, start, depth = w_mid, b * BLOCK - LANES, 2 * BLOCK
                xh = high[0:height, start : start + depth]
                xl = low[0:height, start : start + depth]
                wh, wl = w[level, 0], w[level, 1]
                buf[0:height, b * BLOCK : (b + 1) * BLOCK] = jnp.dot(
                    jnp.concatenate([xh, xl, xh], axis=1),
                    jnp.concatenate([wh, wh, wl], axis=0),
                    preferred_element_type=jnp.float32,
                )

            def rows(i, carry, level=level, s=s):
                lanes = pl.ds(pl.multiple_of(i * LANES, LANES), LANES)
                lane = lax.broadcasted_iota(jnp.int32, (1, LANES), 1)
                on = lane % s == 0
                x = {
                    p: buf[pl.ds(groups * (p // s), groups), lanes] for p in range(0, phases, s)
                }
                index = lax.broadcasted_iota(jnp.int32, (groups, LANES), 0)
                first = jnp.logical_and(index == 0, at_top)
                last = jnp.logical_and(index == inner - 1, at_bottom)
                for number, factor in enumerate(STEPS):
                    c = jnp.where(on, factor, 0.0)
                    if number % 2 == 0:
                        for p in range(s, phases, 2 * s):
                            if p + s < phases:
                                after = x[p + s]
                            else:
                                after = jnp.where(last, x[p - s], pltpu.roll(x[0], groups - 1, 0))
                            x[p] = x[p] + c * (x[p - s] + after)
                    else:
                        for p in range(0, phases, 2 * s):
                            if p > 0:
                                before = x[p - s]
                            else:
                                before = jnp.where(first, x[s], pltpu.roll(x[phases - s], 1, 0))
                            x[p] = x[p] + c * (before + x[p + s])
                up = jnp.where(on, LIFT_ZETA, 1.0)
                down = jnp.where(on, 1.0 / LIFT_ZETA, 1.0)
                for p in x:
                    is_low = p % (2 * s) == 0
                    value = x[p] * (up if is_low else down)
                    if is_low and level < SLEVELS - 1:
                        split(pl.ds(groups * (p // (2 * s)), groups), lanes, value)
                    else:
                        planes[n, p, :, lanes] = value[:inner]
                return carry

            lax.fori_loop(0, width // LANES, rows, 0)

            done = [
                p for p in range(0, phases, s) if p % (2 * s) != 0 or level == SLEVELS - 1
            ]

            order = [phase_at(q) for q in range(phases)]

            def first_frames(to_right, done=done):
                for c in done:
                    if order.index(c) < PAIRED:
                        for r in range(CUTS):
                            i = order.index(c) * CUTS + r
                            source = planes.at[(0,) + spot(i)]
                            if to_right:
                                near(0, i, source).start()
                            elif i < straight:
                                direct(i, source).start()
                            else:
                                far(0, i, source).start()

            @pl.when(both(step == 0, is_right))
            def _(first_frames=first_frames):
                first_frames(True)

            @pl.when(both(step == 0, both(is_left, no(is_first))))
            def _(first_frames=first_frames):
                first_frames(False)

            @pl.when(step != 3)
            def _(done=done):
                for c in done:
                    if order.index(c) >= PAIRED:
                        start_forward(n, order.index(c) - PAIRED)

        @pl.when(step == 2)
        def _():
            def last_frame(i, carry):
                at = (3,) + spot(i)
                planes[at] = planes[at] - 0.5 * planes[(2,) + spot(i)]

                @pl.when(both(is_right, no(is_last)))
                def _():
                    far(0, i, planes.at[(3,) + spot(i)]).start()

                return carry

            lax.fori_loop(0, chunks, last_frame, 0)

        @pl.when(step == 3)
        def _():
            def high_frame(i, carry):
                at = spot(i)
                f0 = planes[(0,) + at]
                o1 = planes[(kept,) + at] - 0.5 * (f0 + planes[(2,) + at])
                result[(kept,) + at] = o1
                planes[(kept,) + at] = f0 + 0.25 * o1

                @pl.when(both(is_left, no(is_first)))
                def _():
                    far(1, i, planes.at[(kept,) + spot(i)]).start()

                return carry

            lax.fori_loop(0, chunks, high_frame, 0)

            def high_group(g, carry):
                c = phase_at(PAIRED + g)
                o1 = planes[kept, c] - 0.5 * (planes[kept - 1, c] + planes[kept + 1, c])
                planes[kept, c] = o1
                result[kept, c] = o1
                start_forward(kept, g)
                return carry

            lax.fori_loop(0, grouped, high_group, 0)

        @pl.when(step == 1)
        def _():
            relay_some(straight, straight + 4)

        @pl.when(step == 2)
        def _():
            relay_some(straight + 4, straight + 10)

        return carry

    lax.fori_loop(0, frames, one_frame, 0)
    acc[...] = jnp.zeros_like(acc)

    total = GROUP * frames

    def send_halo(c):
        arrived(held.at[pl.ds(0, total - frames), c], f_recv.at[c])
        arrived(held.at[pl.ds(0, frames), c], f_own.at[c])

        def strip(i, carry):
            lanes = pl.ds(pl.multiple_of(i * LANES, LANES), LANES)
            left, right = outgoing([held[n, c, :, lanes] for n in range(total)])
            for j in range(TLEVELS):
                to_before[c, j, :, lanes] = left[j]
                to_after[c, j, :, lanes] = right[j]
            return carry

        lax.fori_loop(0, width // LANES, strip, 0)
        start_halos(c)

    def finish(c):
        halo_arrivals(c)

        def strip(i, carry):
            lanes = pl.ds(pl.multiple_of(i * LANES, LANES), LANES)
            f = [held[n, c, :, lanes] for n in range(total)]
            before = [from_before[c, j, :, lanes] for j in range(TLEVELS)]
            after = [from_after[c, j, :, lanes] for j in range(TLEVELS)]
            out = temporal(f, before, after, starts, ends)
            sums = [None] * (TLEVELS + 1)
            for n in range(total):
                if n % frames in moved:
                    held[n, c, :, lanes] = out[n]
                t = level_of(n % 2**TLEVELS, TLEVELS) - 1
                square = out[n] * out[n]
                sums[t] = square if sums[t] is None else sums[t] + square
            return tuple(
                carry[t] + jnp.sum(sums[t].reshape(part // 8, 8, LANES), axis=0)
                for t in range(TLEVELS + 1)
            )

        zero = jnp.zeros((8, LANES), jnp.float32)
        sums = lax.fori_loop(0, width // LANES, strip, (zero,) * (TLEVELS + 1))
        for t in range(TLEVELS + 1):
            acc[phase_at(PAIRED + c), t] = sums[t]
        for i in range(len(moved)):
            back_own(i, c).start()

    def give_back(c):
        for i in range(len(moved)):
            for k in range(GROUP - 1):
                back(i, c, k).start()

    def count_in(n, t, i):
        c, rows = spot(i)
        value = result[n, c, rows, :]
        square = value * value
        folded = sum(square[:, k : k + LANES] for k in range(0, width, LANES))
        acc[c, t] += jnp.sum(folded.reshape(cut // 8, 8, LANES), axis=0)

    def loop(start, stop, body):
        def step(i, carry):
            body(i)
            return carry

        lax.fori_loop(start, stop, step, 0)

    lag = 4

    def halves(i):
        at = spot(i)
        return planes[(2,) + at], result[(1,) + at], result[(3,) + at], planes[(1,) + at]

    def third(i, after):
        at = spot(i)
        result[(3,) + at] = planes[(3,) + at] - 0.5 * after

    @pl.when(is_left)
    def _():
        def highs(i):
            third(i, take_near(0, i))

        def relays(i):
            @pl.when(no(is_last))
            def _():
                relay(i, 0)

        def questions(i):
            o3 = result[(3,) + spot(i)]
            made[(1,) + slot(i)] = 0.25 * o3

            @pl.when(no(is_last))
            def _():
                made[(1,) + slot(i)] = 0.25 * result[(3,) + spot(i)] + take_far(1, i)

            near(1, i, made.at[(1,) + slot(i)]).start()

        ahead = straight + 14
        loop(straight + 10, ahead, relays)
        loop(0, chunks - ahead, lambda i: (relays(i + ahead), highs(i)))
        loop(chunks - ahead, chunks, highs)
        loop(0, chunks, questions)

    @pl.when(is_right)
    def _():
        def highs(i):
            at = spot(i)

            @pl.when(is_last)
            def _():
                third(i, planes[(2,) + at])

            @pl.when(no(is_last))
            def _():
                third(i, take_near(0, i))

        def answer_highs(i):
            made[(0,) + slot(i)] = planes[(1,) + spot(i)]

            @pl.when(no(is_first))
            def _():
                made[(0,) + slot(i)] = planes[(1,) + spot(i)] + 0.25 * take_far(0, i)

            near(1, i, made.at[(0,) + slot(i)]).start()

        def highs_and_answers(i):
            highs(i)
            answer_highs(i - lag)

        loop(0, lag, highs)
        loop(lag, chunks, highs_and_answers)
        loop(chunks - lag, chunks, answer_highs)

    loop(0, grouped, send_halo)

    def left_seconds(i):
        at = spot(i)
        f2, o1, o3, h = halves(i)
        start = jnp.where(is_first, 0.125 * o1, -0.0625 * planes[(0,) + at])
        p2 = f2 + 0.25 * (o1 + o3) - 0.5 * h - 0.125 * o3 - start
        p2 = p2 - 0.5 * take_near(1, i)
        result[(2,) + at] = p2
        made[(2,) + slot(i)] = h + 0.25 * p2

        @pl.when(no(is_first))
        def _():
            far(2, i, made.at[(2,) + slot(i)]).start()

    def right_seconds(i):
        at = spot(i)
        f2, o1, o3, h = halves(i)
        came = take_near(1, i)
        p2 = f2 + 0.25 * (o1 + o3)
        p2 = p2 - jnp.where(is_last, h + came, 0.5 * (h + came) + 0.125 * o3)
        result[(2,) + at] = p2
        made[(1,) + slot(i)] = 0.25 * (o3 + p2)

        @pl.when(no(is_last))
        def _():
            far(1, i, made.at[(1,) + slot(i)]).start()

    def seconds(j):
        @pl.when(is_left)
        def _():
            loop(j * CUTS, (j + 1) * CUTS, left_seconds)

        @pl.when(is_right)
        def _():
            loop(j * CUTS, (j + 1) * CUTS, right_seconds)

    loop(0, PAIRED, seconds)
    loop(0, grouped, finish)

    def sums_so_far(i):
        count_in(1, 0, i)
        count_in(3, 0, i)
        count_in(2, 1, i)

    @pl.when(is_left)
    def _():
        def thirds(i):
            f2, o1, o3, h = halves(i)
            p2 = result[(2,) + spot(i)]
            own = 0.25 * (o3 + p2) - jnp.where(is_last, 1.0, 0.5) * made[(2,) + slot(i)]
            made[(3,) + slot(i)] = own - jnp.where(is_first, 0.125, 0.0) * (o1 + p2)

            @pl.when(no(is_last))
            def _():
                made[(3,) + slot(i)] -= 0.5 * take_far(2, i)

            near(2, i, made.at[(3,) + slot(i)]).start()

        loop(0, 0, give_back)
        loop(0, chunks, thirds)
        loop(0, grouped, give_back)

        loop(0, chunks, sums_so_far)

        def lows(i):
            at = spot(i)
            start = jnp.where(is_first, 0.25, 0.0) * (result[(1,) + at] + result[(2,) + at])
            result[(0,) + at] = made[(2,) + slot(i)] + start + take_near(2, i)
            count_in(0, 3, i)

        loop(0, chunks, lows)

    @pl.when(is_right)
    def _():
        def thirds(i):
            at = spot(i)
            mine = made[(1,) + slot(i)]
            scale = jnp.where(is_last, 0.0, 0.5)
            result[(0,) + at] = (
                planes[(1,) + at] + 0.25 * result[(2,) + at] - scale * mine
            )

            @pl.when(no(is_first))
            def _():
                result[(0,) + at] -= jnp.where(is_last, 1.0, 0.5) * take_far(1, i)

            d = result[(0,) + at] + take_near(2, i)
            result[(0,) + at] = d
            count_in(0, 2, i)
            made[(2,) + slot(i)] = mine + 0.25 * d

            @pl.when(no(is_last))
            def _():
                far(2, i, made.at[(2,) + slot(i)]).start()

        def answer_thirds(i):
            made[(3,) + slot(i)] = jnp.where(is_first, 0.5, 0.25) * result[(0,) + spot(i)]

            @pl.when(no(is_first))
            def _():
                made[(3,) + slot(i)] += take_far(2, i)

            near(2, i, made.at[(3,) + slot(i)]).start()

        def thirds_and_answers(i):
            thirds(i)
            answer_thirds(i - lag)

        loop(0, 1, give_back)
        loop(0, chunks, sums_so_far)
        loop(0, lag, thirds)
        loop(lag, chunks, thirds_and_answers)
        loop(chunks - lag, chunks, answer_thirds)
        loop(1, grouped, give_back)

    lane = lax.broadcasted_iota(jnp.int32, (1, LANES), 1)
    packed[...] = jnp.zeros_like(packed)
    for t in range(TLEVELS + 1):
        line = jnp.zeros((1, LANES), jnp.float32)
        for u in range(1, SLEVELS + 2):
            mine = sum(acc[c, t] for c in range(phases) if level_of(c, SLEVELS) == u)
            mine = jnp.sum(mine, axis=0, keepdims=True)
            distance = PERIOD
            while distance < LANES:
                mine = mine + pltpu.roll(mine, distance, 1)
                distance = 2 * distance
            line = jnp.where(lane // (LANES // (SLEVELS + 1)) == u - 1, mine, line)
        packed[pl.ds(t, 1), :] = line

    def to_other(j):
        return pltpu.make_async_remote_copy(
            src_ref=packed,
            dst_ref=inbox.at[flat],
            send_sem=s_send,
            recv_sem=s_recv,
            device_id=place((flat + j) % all_devices),
            device_id_type=MESH,
        )

    def start_sums(j, carry):
        to_other(j).start()
        return carry

    lax.fori_loop(1, all_devices, start_sums, 0)
    inbox[flat] = packed[...]

    arrived(inbox.at[pl.ds(0, all_devices - 1)], s_recv)
    sums = lax.fori_loop(1, all_devices, lambda j, s: s + inbox[j], inbox[0])
    counted = float(count * frames * strips * inner * phases * width)
    band, share = energy_tables(counted)
    energy[...] = share * jnp.dot(
        sums, band, precision=lax.Precision.HIGHEST, preferred_element_type=jnp.float32
    )

    arrived(inbox.at[pl.ds(0, all_devices - 1)], s_send)
    for k in range(GROUP - 1):
        arrived(held.at[pl.ds(0, frames)], f_send.at[k])
        arrived(held.at[pl.ds(0, len(moved))], r_send.at[k])
        arrived(held.at[pl.ds(0, len(moved))], r_recv.at[k])
    arrived(held.at[pl.ds(0, len(moved))], r_own)

    @pl.when(jnp.logical_not(starts))
    def _():
        arrived(to_before, h_send.at[0])

    @pl.when(jnp.logical_not(ends))
    def _():
        arrived(to_after, h_send.at[1])

    for kind in (1, 2):
        arrived(near_in.at[kind], n_send.at[kind])

    @pl.when(is_right)
    def _():
        arrived(near_in.at[0], n_send.at[0])

    @pl.when(both(is_left, no(is_last)))
    def _():
        arrived(near_in.at[0, pl.ds(0, PAIRED - DIRECT)], n_send.at[0])

    @pl.when(jnp.logical_or(both(is_left, no(is_first)), both(is_right, no(is_last))))
    def _():
        for kind in (1, 2):
            arrived(far_in.at[kind], p_send.at[kind])

    @pl.when(both(is_left, no(is_first)))
    def _():
        arrived(near_in.at[0, pl.ds(0, DIRECT)], d_send)
        arrived(far_in.at[0, pl.ds(0, PAIRED - DIRECT)], p_send.at[0])

    @pl.when(both(is_right, no(is_last)))
    def _():
        arrived(far_in.at[0], p_send.at[0])

    @pl.when(jnp.logical_not(at_bottom))
    def _():
        arrived(edges.at[:, :, pl.ds(MARGIN, MARGIN), :], e_send.at[0])

    @pl.when(jnp.logical_not(at_top))
    def _():
        arrived(edges.at[:, :, pl.ds(0, MARGIN), :], e_send.at[1])


def weave_kernel(planes, energy, o_ref, e_ref, sem):
    frames, phases = planes.shape[:2]
    for n in range(frames):
        for p in range(phases):
            pltpu.make_async_copy(planes.at[n, p], o_ref.at[n, :, p, :], sem).start()
    e_ref[...] = energy[: TLEVELS + 1, : 3 * SLEVELS + 1]
    pltpu.make_async_copy(planes, planes, sem).wait()


def shards(footage):
    frames, rows, width = footage.shape
    inner = rows // PERIOD
    groups = inner + 2 * MARGIN
    strips = lax.axis_size("row")
    devices = lax.axis_size("frame") * strips
    any_space = pl.BlockSpec(memory_space=pl.ANY)
    vmem = pl.BlockSpec(memory_space=pltpu.VMEM)
    f32, bf16 = jnp.float32, jnp.bfloat16
    traffic = pltpu.VMEM((3, PAIRED, inner, width), f32)
    chunks = PAIRED * CUTS
    grouped = PERIOD - PAIRED
    part = inner // GROUP
    halo_buffer = pltpu.VMEM((grouped, TLEVELS, part, width), f32)
    dma = pltpu.SemaphoreType.DMA
    planes, energy = pl.pallas_call(
        video_kernel,
        out_shape=(
            jax.ShapeDtypeStruct((frames, PERIOD, inner, width), f32),
            jax.ShapeDtypeStruct((8, LANES), f32),
        ),
        in_specs=[any_space, pl.BlockSpec(memory_space=pltpu.HBM)],
        out_specs=(vmem, vmem),
        scratch_shapes=[
            pltpu.VMEM((frames, PERIOD, inner, width), f32),
            pltpu.VMEM((frames, PERIOD, 2 * MARGIN, width), f32),
            pltpu.VMEM((PERIOD * groups, width), bf16),
            pltpu.VMEM((PERIOD * groups, width), bf16),
            pltpu.VMEM((PERIOD * groups, width), f32),
            pltpu.VMEM((SLEVELS, 2, 2 * BLOCK, BLOCK), bf16),
            pltpu.VMEM((SLEVELS, 2, BLOCK + LANES, BLOCK), bf16),
            pltpu.VMEM((SLEVELS, 2, BLOCK + LANES, BLOCK), bf16),
            traffic,
            traffic,
            pltpu.VMEM((4, PAIRED, inner, width), f32),
            pltpu.VMEM((GROUP * frames, grouped, part, width), f32),
            halo_buffer, halo_buffer, halo_buffer, halo_buffer,
            pltpu.VMEM((PERIOD, TLEVELS + 1, 8, LANES), f32),
            pltpu.VMEM((8, LANES), f32),
            pltpu.VMEM((devices, 8, LANES), f32),
            dma((frames,)), dma((SLEVELS, 3)),
            dma((2,)), dma((2, frames)),
            dma((3,)), dma((3, chunks)), dma((3,)), dma((3, chunks)), dma,
            dma((GROUP - 1,)), dma((grouped,)), dma((grouped,)),
            dma((2,)), dma((2, grouped)),
            dma((GROUP - 1,)), dma((GROUP - 1,)), dma,
            dma, dma,
        ],
        compiler_params=pltpu.CompilerParams(
            collective_id=0, has_side_effects=True, vmem_limit_bytes=44 * 2**20
        ),
    )(
        footage.reshape(frames, inner, PERIOD, width),
        jnp.asarray(column_weights(width)),
    )
    coeffs, means = pl.pallas_call(
        weave_kernel,
        out_shape=(
            jax.ShapeDtypeStruct((frames, inner, PERIOD, width), f32),
            jax.ShapeDtypeStruct((TLEVELS + 1, 3 * SLEVELS + 1), f32),
        ),
        in_specs=[vmem, vmem],
        out_specs=(any_space, vmem),
        scratch_shapes=[dma],
        compiler_params=pltpu.CompilerParams(vmem_limit_bytes=20 * 2**20),
    )(planes, energy)
    return coeffs.reshape(frames, rows, width), means


def solution(mesh):
    return jax.shard_map(
        shards,
        mesh=mesh,
        in_specs=(P("frame", "row", None),),
        out_specs=(P("frame", "row", None), P()),
        check_vma=False,
    )
```
